256 devices in a mesh: gx: 32 (over x, z), gy: 8 (over y, core).
Axes of the slice: x: 4, y: 4, z: 8, core: 2. Of those that a mesh axis runs over, the one named last changes fastest.
Arguments:
- dense_grads: float32 [256, 2048, 1024], P(('gx', 'gy')), may hold values from -24 to 24
- dense_param: float32 [2048, 1024], P(('gx', 'gy')), may hold values from -6 to 6
- dense_acc: float32 [2048, 1024], P(('gx', 'gy'))
- table: float32 [1048576, 128], P(('gx', 'gy')), may hold values from -6 to 6
- row_acc: float32 [1048576], P(('gx', 'gy'))
- touched: int32 [131072], P(('gx', 'gy')), may hold values from 0 to 4095, as said below
- emb_grads: float32 [131072, 128], P(('gx', 'gy'))
Outputs:
- new_dense: float32 [2048, 1024], P(('gx', 'gy'))
- new_dense_acc: float32 [2048, 1024], P(('gx', 'gy'))
- new_table: float32 [1048576, 128], P(('gx', 'gy'))
- new_row_acc: float32 [1048576], P(('gx', 'gy'))
The draws below stay inside these ranges and needn't reach their ends.
Inputs may be any that keep to these rules, and one draw needn't show every extreme that they name: `touched`: within one device's 512 entries no row number repeats.
All inputs are finite; a program needn't handle non-finite values.
Results may differ from the reference program's by a relative error of at most 0.000022.
Values sent between devices are 32-bit elements; how exact they have to be, the bound alone decides.
A program may use at most 128 MiB of HBM per device.

```python
import jax
import jax.numpy as jnp
from jax import lax

H = 1024
EMB_DIM = 128
ROWS_DEV = 4096
TOUCH_DEV = 512
SHARDS = 256
DENSE_ROWS = 2048
TABLE_ROWS = 1048576
TOUCHED = 131072


def draw_touched(key, part):
    keys = jax.random.split(jax.random.fold_in(key, 11), SHARDS)
    picks = jax.vmap(lambda single: jax.random.permutation(single, ROWS_DEV)[:TOUCH_DEV])(keys)
    return picks.reshape(TOUCHED).astype(jnp.int32)


def draw_emb_grads(key, part):
    first = jax.random.fold_in(jax.random.fold_in(key, 23), 0)
    owner = jnp.arange(TOUCHED, dtype=jnp.float32) // TOUCH_DEV
    ramp = 1.0 + 2.0 * owner / max(SHARDS - 1, 1)
    values = jax.random.normal(first, (TOUCHED, EMB_DIM), jnp.float32)
    scale = ramp / (8.0 * jnp.sqrt(jnp.float32(SHARDS)))
    return (values * scale[:, None]).astype(jnp.float32)


def draw_dense_acc(key, part):
    logs = jax.random.uniform(jax.random.fold_in(key, 37), (DENSE_ROWS, H), jnp.float32, jnp.log(0.0005), jnp.log(0.05))
    return (jnp.exp(logs) / jnp.float32(SHARDS)).astype(jnp.float32)


def draw_row_acc(key, part):
    logs = jax.random.uniform(jax.random.fold_in(key, 41), (TABLE_ROWS,), jnp.float32, jnp.log(1e-05), jnp.log(0.001))
    return (jnp.exp(logs) / jnp.float32(SHARDS)).astype(jnp.float32)


def spiked(drawn, rng, source, target, shards_of, factor):
    owner, partner = [(jnp.arange(drawn.shape[dim]) // (drawn.shape[dim] // shards_of)).reshape([-1 if axis == dim else 1 for axis in range(drawn.ndim)]) for dim in (source, target)]
    chosen = jax.random.permutation(rng, shards_of)[partner]
    strong = (owner == chosen) | (owner == (partner + shards_of // 2) % shards_of)
    return jnp.where(strong, factor * drawn, drawn)


def steps_of(key, dims, cuts, smallest, top_value):
    loudness, own = 1.0, jax.random.fold_in(key, 6)
    for position, shards_of in cuts:
        heights = jnp.exp(jax.random.uniform(jax.random.fold_in(own, position), (shards_of,), jnp.float32, smallest / len(cuts), top_value / len(cuts)))
        loudness = loudness * jnp.repeat(heights, dims[position] // shards_of).reshape([-1 if axis == position else 1 for axis in range(len(dims))])
    return loudness


def centred(stream_key, shape, scale, most, pieces=(), kind=jnp.bfloat16):
    drawn = scale * jax.random.normal(stream_key, shape, jnp.float32)
    if pieces:
        drawn = drawn * steps_of(stream_key, shape, pieces, -0.22, 0.18)
    return jnp.clip(drawn, -most, most).astype(kind)


def noise_with(rng, dims, scale, most, cuts, heavy, kind=jnp.bfloat16):
    result = scale * jax.random.normal(rng, dims, jnp.float32)
    if cuts:
        result = result * steps_of(rng, dims, cuts, -0.22, 0.18)
    return jnp.clip(spiked(result, jax.random.fold_in(rng, 3), *heavy), -most, most).astype(kind)


def setup_inputs(seed: int = 0) -> dict:
    key_list = jax.random.split(jax.random.key(seed), 8)
    return {
        "dense_grads": noise_with(key_list[0], (SHARDS, DENSE_ROWS, H), 1.0, 24.0, ((0, 256),), (0, 1, 256, 6.0), jnp.float32),
        "dense_param": centred(key_list[1], (DENSE_ROWS, H), 1.0, 6.0, ((0, 256),), jnp.float32),
        "dense_acc": draw_dense_acc(jax.random.fold_in(key_list[7], 71), 0),
        "table": centred(key_list[3], (TABLE_ROWS, EMB_DIM), 1.0, 6.0, ((0, 256),), jnp.float32),
        "row_acc": draw_row_acc(jax.random.fold_in(key_list[7], 71), 0),
        "touched": draw_touched(jax.random.fold_in(key_list[7], 71), 0),
        "emb_grads": draw_emb_grads(jax.random.fold_in(key_list[7], 71), 0),
    }


learn_rate = 0.5
max_norm = 8.0
epsilon = 1e-10

def reference(dense_grads, dense_param, dense_acc, table, row_acc, touched, emb_grads):
    mean_grad = lax.optimization_barrier(jnp.sum(dense_grads, axis=0)) / jnp.float32(SHARDS)
    norm_sq = jnp.sum(mean_grad * mean_grad) + jnp.sum(emb_grads * emb_grads)
    clip = jnp.minimum(jnp.float32(1.0), max_norm / (jnp.sqrt(norm_sq) + 1e-06))
    scaled = clip * mean_grad
    new_dense_acc = dense_acc + scaled * scaled
    new_dense = dense_param - learn_rate * scaled / (jnp.sqrt(new_dense_acc) + epsilon)
    owner = (jnp.arange(TOUCHED, dtype=jnp.int32) // TOUCH_DEV).astype(jnp.int32)
    global_rows = (owner * ROWS_DEV + touched).astype(jnp.int32)
    row_grads = clip * emb_grads
    square_mean = lax.optimization_barrier(jnp.mean(row_grads * row_grads, axis=1))
    updated_acc = row_acc[global_rows] + square_mean
    new_row_acc = row_acc.at[global_rows].set(updated_acc)
    updated_rows = table[global_rows] - learn_rate * row_grads / (jnp.sqrt(updated_acc) + epsilon)[:, None]
    new_table = table.at[global_rows].set(updated_rows)
    return (new_dense, new_dense_acc, new_table, new_row_acc)
```

```python
import functools

import jax
import jax.numpy as jnp
from jax import lax
from jax.experimental import pallas as pl
from jax.experimental.pallas import tpu as pltpu
from jax.sharding import PartitionSpec as P

learn_rate = 0.5
max_norm = 8.0
epsilon = 1e-10

MESH = pl.DeviceIdType.MESH
NX, NZ, NY, NC = 4, 8, 4, 2
SHARDS = 256
XS, YS, ZS = 3, 3, 2
UNITS = XS + YS + ZS
LANES = 128
F32 = jnp.float32


class Sends:
    def __init__(self, send_sems, recv_sems):
        self.send_sems, self.recv_sems = send_sems, recv_sems
        self.made = {}

    def start(self, name, src, dst, device):
        slot = len(self.made)
        copy = pltpu.make_async_remote_copy(
            src_ref=src,
            dst_ref=dst,
            send_sem=self.send_sems.at[slot],
            recv_sem=self.recv_sems.at[slot],
            device_id=device,
            device_id_type=MESH,
        )
        copy.start()
        self.made[name] = copy

    def wait(self, name):
        self.made[name].wait_recv()

    def drain(self):
        for copy in self.made.values():
            copy.wait_send()


def reduce_kernel(
    g_ref, e_ref, mean_ref, norm_ref,
    acc, pair, emb,
    a_relay, a_last, a_mid, a_end,
    b_relay, b_last, b_mid, b_end,
    c_far, c_chain, c_mid, c_end,
    n_own, n_one, n_sum, n_two,
    send_sems, recv_sems, load_sems,
):
    gx, gy = lax.axis_index("gx"), lax.axis_index("gy")
    x, z = gx // NZ, gx % NZ
    y, c = gy // NC, gy % NC

    def dev(dx=0, dy=0, dz=0, core=None):
        return (
            ((x + dx) % NX) * NZ + (z + dz) % NZ,
            ((y + dy) % NY) * NC + (c if core is None else core),
        )

    def dev_zc(k):
        q = (z * NC + c + k) % (NZ * NC)
        return (x * NZ + q // NC, y * NC + q % NC)

    def dev_xy(k):
        q = (x * NY + y + k) % (NX * NY)
        return ((q // NY) * NZ + z, (q % NY) * NC + c)

    cols = lambda u: pl.ds(u * LANES, LANES)
    order = [0, 3, 6, 1, 4, 7, 2, 5]
    loads = {}
    for u in order:
        loads[u] = pltpu.make_async_copy(
            g_ref.at[:, :, :, c, :, cols(u)], acc.at[u], load_sems.at[u]
        )
        loads[u].start()
    load_emb = pltpu.make_async_copy(e_ref, emb, load_sems.at[UNITS])
    load_emb.start()

    barrier = pltpu.get_barrier_semaphore()
    for k in range(1, 16):
        pl.semaphore_signal(barrier, inc=1, device_id=dev_zc(k), device_id_type=MESH)
        pl.semaphore_signal(barrier, inc=1, device_id=dev_xy(k), device_id_type=MESH)
    pl.semaphore_wait(barrier, 30)

    net = Sends(send_sems, recv_sems)
    other = 1 - c
    mate = dev(core=other)

    def part(ref, u, kind, k):
        if kind == "x":
            return ref.at[u, (x + k) % NX]
        if kind == "y":
            return ref.at[u, :, :, (y + k) % NY]
        return ref.at[u, :, (z + k) % NZ]

    def give(u, kind, k):
        if kind == "x":
            src = g_ref.at[(x + k) % NX, :, :, other, :, cols(u)]
        elif kind == "y":
            src = g_ref.at[:, :, (y + k) % NY, other, :, cols(u)]
        else:
            src = g_ref.at[:, (z + k) % NZ, :, other, :, cols(u)]
        net.start(("pair", u, k), src, part(pair, u, kind, k), mate)

    kinds = {u: "x" if u < XS else "y" if u < XS + YS else "z" for u in range(UNITS)}
    waves = [[0, 3, 6], [1, 4, 7], [2, 5]]
    far_of = {"x": [2], "y": [2], "z": [4]}
    near_of = {"x": [1, 3, 0], "y": [1, 3, 0], "z": [3, 5, 2, 6, 1, 7, 0]}
    for wave in waves:
        for u in wave:
            for k in far_of[kinds[u]]:
                give(u, kinds[u], k)
        for u in wave:
            for k in near_of[kinds[u]]:
                give(u, kinds[u], k)

    def take(u, k):
        kind = kinds[u]
        net.wait(("pair", u, k))
        mine = part(acc, u, kind, k)
        mine[...] = mine[...] + part(pair, u, kind, k)[...]

    loaded = set()

    def load(u):
        if u not in loaded:
            loaded.add(u)
            loads[u].wait()

    LO, HI = pl.ds(0, 4), pl.ds(4, 4)

    def a_part(u, k, half):
        return acc.at[u, (x + k) % NX, half]

    def a_far(w):
        u = w
        load(u)
        take(u, 2)
        net.start(("ar", w), a_part(u, 2, LO), a_relay.at[w, 0], dev(dx=1))
        net.start(("al", w), a_part(u, 2, HI), a_relay.at[w, 1], dev(dx=-1))

    def a_near(w):
        u = w
        take(u, 1)
        net.start(("aer", w), a_part(u, 1, HI), a_last.at[w, 0, HI], dev(dx=1))
        take(u, 3)
        net.start(("ael", w), a_part(u, 3, LO), a_last.at[w, 1, LO], dev(dx=-1))
        take(u, 0)

    def a_late(w):
        u = w
        net.wait(("ar", w))
        ref = a_part(u, 1, LO)
        ref[...] = ref[...] + a_relay[w, 0]
        net.start(("alr", w), ref, a_last.at[w, 0, LO], dev(dx=1))
        net.wait(("al", w))
        ref = a_part(u, 3, HI)
        ref[...] = ref[...] + a_relay[w, 1]
        net.start(("all", w), ref, a_last.at[w, 1, HI], dev(dx=-1))

    def a_two(w):
        u = w
        for name in ("aer", "ael", "alr", "all"):
            net.wait((name, w))
        ref = acc.at[u, x]
        ref[...] = ref[...] + (a_last[w, 0] + a_last[w, 1])
        for k in (2, 1, 3):
            net.start(("am", w, k), acc.at[u, x, :, (y + k) % NY], a_mid.at[w, k - 1], dev(dy=k))

    def a_three(w):
        u = w
        for k in (1, 3, 2):
            net.wait(("am", w, k))
        ref = acc.at[u, x, :, y]
        ref[...] = ref[...] + (a_mid[w, 0] + a_mid[w, 1] + a_mid[w, 2])
        for k in (4, 3, 5, 2, 6, 1, 7):
            net.start(("ae", w, k), acc.at[u, x, (z + k) % NZ, y], a_end.at[w, k - 1], dev(dz=k))

    def b_part(u, k, half):
        return acc.at[u, :, half, (y + k) % NY]

    def b_far(w):
        u = XS + w
        load(u)
        take(u, 2)
        net.start(("br", w), b_part(u, 2, LO), b_relay.at[w, 0], dev(dy=1))
        net.start(("bl", w), b_part(u, 2, HI), b_relay.at[w, 1], dev(dy=-1))

    def b_near(w):
        u = XS + w
        take(u, 1)
        net.start(("ber", w), b_part(u, 1, HI), b_last.at[w, 0, :, HI], dev(dy=1))
        take(u, 3)
        net.start(("bel", w), b_part(u, 3, LO), b_last.at[w, 1, :, LO], dev(dy=-1))
        take(u, 0)

    def b_late(w):
        u = XS + w
        net.wait(("br", w))
        ref = b_part(u, 1, LO)
        ref[...] = ref[...] + b_relay[w, 0]
        net.start(("blr", w), ref, b_last.at[w, 0, :, LO], dev(dy=1))
        net.wait(("bl", w))
        ref = b_part(u, 3, HI)
        ref[...] = ref[...] + b_relay[w, 1]
        net.start(("bll", w), ref, b_last.at[w, 1, :, HI], dev(dy=-1))

    def b_two(w):
        u = XS + w
        for name in ("ber", "bel", "blr", "bll"):
            net.wait((name, w))
        ref = acc.at[u, :, :, y]
        ref[...] = ref[...] + (b_last[w, 0] + b_last[w, 1])
        for k in (2, 1, 3):
            net.start(("bm", w, k), acc.at[u, (x + k) % NX, :, y], b_mid.at[w, k - 1], dev(dx=k))

    def b_three(w):
        u = XS + w
        for k in (1, 3, 2):
            net.wait(("bm", w, k))
        ref = acc.at[u, x, :, y]
        ref[...] = ref[...] + (b_mid[w, 0] + b_mid[w, 1] + b_mid[w, 2])
        for k in (4, 3, 5, 2, 6, 1, 7):
            net.start(("be", w, k), acc.at[u, x, (z + k) % NZ, y], b_end.at[w, k - 1], dev(dz=k))

    XLO, XHI = pl.ds(0, 2), pl.ds(2, 2)

    def c_part(u, k, half=slice(None)):
        return acc.at[u, half, (z + k) % NZ]

    def c_zero(w):
        u = XS + YS + w
        load(u)
        take(u, 4)
        net.start(("c1r", w), c_part(u, 4, XLO), c_far.at[w, 0], dev(dz=1))
        net.start(("c1l", w), c_part(u, 4, XHI), c_far.at[w, 1], dev(dz=-1))

    def c_near(w):
        u = XS + YS + w
        take(u, 3)
        net.start(("c2er", w), c_part(u, 3, XHI), c_chain.at[w, 0, 0, XHI], dev(dz=1))
        take(u, 5)
        net.start(("c2el", w), c_part(u, 5, XLO), c_chain.at[w, 1, 0, XLO], dev(dz=-1))
        for k in (2, 6, 1, 7, 0):
            take(u, k)

    def c_one(w):
        u = XS + YS + w
        net.wait(("c1r", w))
        ref = c_part(u, 3, XLO)
        ref[...] = ref[...] + c_far[w, 0]
        net.start(("c2lr", w), ref, c_chain.at[w, 0, 0, XLO], dev(dz=1))
        net.wait(("c1l", w))
        ref = c_part(u, 5, XHI)
        ref[...] = ref[...] + c_far[w, 1]
        net.start(("c2ll", w), ref, c_chain.at[w, 1, 0, XHI], dev(dz=-1))

    def c_two(w):
        u = XS + YS + w
        net.wait(("c2er", w))
        net.wait(("c2lr", w))
        ref = c_part(u, 2)
        ref[...] = ref[...] + c_chain[w, 0, 0]
        net.start(("c3r", w), ref, c_chain.at[w, 0, 1], dev(dz=1))
        net.wait(("c2el", w))
        net.wait(("c2ll", w))
        ref = c_part(u, 6)
        ref[...] = ref[...] + c_chain[w, 1, 0]
        net.start(("c3l", w), ref, c_chain.at[w, 1, 1], dev(dz=-1))

    def c_three(w):
        u = XS + YS + w
        net.wait(("c3r", w))
        ref = c_part(u, 1)
        ref[...] = ref[...] + c_chain[w, 0, 1]
        net.start(("c4r", w), ref, c_chain.at[w, 0, 2], dev(dz=1))
        net.wait(("c3l", w))
        ref = c_part(u, 7)
        ref[...] = ref[...] + c_chain[w, 1, 1]
        net.start(("c4l", w), ref, c_chain.at[w, 1, 2], dev(dz=-1))

    def c_four(w):
        u = XS + YS + w
        net.wait(("c4r", w))
        net.wait(("c4l", w))
        ref = acc.at[u, :, z]
        ref[...] = ref[...] + (c_chain[w, 0, 2] + c_chain[w, 1, 2])
        for k in (2, 1, 3):
            net.start(("cm", w, k), acc.at[u, (x + k) % NX, z], c_mid.at[w, k - 1], dev(dx=k))

    def c_five(w):
        u = XS + YS + w
        for k in (1, 3, 2):
            net.wait(("cm", w, k))
        ref = acc.at[u, x, z]
        ref[...] = ref[...] + (c_mid[w, 0] + c_mid[w, 1] + c_mid[w, 2])
        for k in (2, 1, 3):
            net.start(("ce", w, k), acc.at[u, x, z, (y + k) % NY], c_end.at[w, k - 1], dev(dy=k))

    squares = []

    def end(u, name, w, ends, ks):
        total = acc[u, x, z, y]
        for k in ks:
            net.wait((name, w, k))
            total = total + ends[w, k - 1]
        mean = total / F32(SHARDS)
        mean_ref[:, cols(u)] = mean
        squares.append(mean * mean)

    def a_end_step(w):
        end(w, "ae", w, a_end, (1, 7, 2, 6, 3, 5, 4))

    def b_end_step(w):
        end(XS + w, "be", w, b_end, (1, 7, 2, 6, 3, 5, 4))

    def c_end_step(w):
        end(XS + YS + w, "ce", w, c_end, (1, 3, 2))

    a_far(0); b_far(0); c_zero(0)
    a_near(0); b_near(0); c_near(0)
    a_far(1); b_far(1); c_zero(1)
    c_one(0); a_late(0); b_late(0)
    a_near(1); b_near(1); c_near(1)
    a_far(2); b_far(2)
    load_emb.wait()
    grads = emb[...]
    squares.append(jnp.sum((grads * grads).reshape(-1, 8, LANES), axis=0))
    c_two(0)
    c_one(1)
    a_late(1); b_late(1)
    a_near(2); b_near(2)
    a_two(0); b_two(0)
    c_three(0); c_two(1)
    a_late(2); b_late(2)
    a_two(1); b_two(1)
    a_three(0); b_three(0)
    c_four(0); c_three(1)
    a_three(1); b_three(1)
    a_end_step(0); b_end_step(0)
    a_two(2); b_two(2)
    c_five(0); c_four(1)
    c_end_step(0)
    a_end_step(1); b_end_step(1)
    a_three(2); b_three(2)
    c_five(1)
    c_end_step(1)
    a_end_step(2); b_end_step(2)

    total = functools.reduce(lambda p, q: p + q, squares)
    n_own[...] = jnp.sum(total, axis=0, keepdims=True)
    for k in range(1, 16):
        net.start(("n1", k), n_own, n_one.at[k - 1], dev_zc(k))
    line = n_own[...]
    for k in range(1, 16):
        net.wait(("n1", k))
    for k in range(1, 16):
        line = line + n_one[k - 1]
    n_sum[...] = line
    for k in range(1, 16):
        net.start(("n2", k), n_sum, n_two.at[k - 1], dev_xy(k))
    for k in range(1, 16):
        net.wait(("n2", k))
    for k in range(1, 16):
        line = line + n_two[k - 1]
    norm_ref[...] = line
    net.drain()


def reduce_mean(grads, emb):
    vm = lambda *shape: pltpu.VMEM(shape + (8, LANES), F32)
    row = lambda *shape: pltpu.VMEM(shape + (1, LANES), F32)
    copies = 4 * (XS + YS) + 8 * ZS + 16 * (XS + YS) + 16 * ZS + 30
    return pl.pallas_call(
        reduce_kernel,
        name="reduce_mean",
        out_shape=(
            jax.ShapeDtypeStruct((8, 1024), F32),
            jax.ShapeDtypeStruct((1, LANES), F32),
        ),
        in_specs=[pl.BlockSpec(memory_space=pl.ANY)] * 2,
        out_specs=(
            pl.BlockSpec(memory_space=pltpu.VMEM),
            pl.BlockSpec(memory_space=pltpu.VMEM),
        ),
        scratch_shapes=[
            vm(UNITS, NX, NZ, NY),
            vm(UNITS, NX, NZ, NY),
            pltpu.VMEM(emb.shape, F32),
            vm(XS, 2, 4, NY), vm(XS, 2, NZ, NY), vm(XS, 3, NZ), vm(XS, 7),
            vm(YS, 2, NX, 4), vm(YS, 2, NX, NZ), vm(YS, 3, NZ), vm(YS, 7),
            vm(ZS, 2, 2, NY), vm(ZS, 2, 3, NX, NY), vm(ZS, 3, NY), vm(ZS, 3),
            row(), row(15), row(), row(15),
            pltpu.SemaphoreType.DMA((copies,)),
            pltpu.SemaphoreType.DMA((copies,)),
            pltpu.SemaphoreType.DMA((UNITS + 1,)),
        ],
        compiler_params=pltpu.CompilerParams(
            collective_id=0, has_side_effects=True, vmem_limit_bytes=24 * 1024 * 1024
        ),
    )(grads.reshape(NX, NZ, NY, NC, 8, 1024), emb)


def body(dense_grads, dense_param, dense_acc, table, row_acc, touched, emb_grads):
    mean_grad, norm_line = reduce_mean(dense_grads, emb_grads)
    norm_sq = jnp.sum(norm_line)
    clip = jnp.minimum(jnp.float32(1.0), max_norm / (jnp.sqrt(norm_sq) + 1e-06))
    scaled = clip * mean_grad
    new_dense_acc = dense_acc + scaled * scaled
    new_dense = dense_param - learn_rate * scaled / (jnp.sqrt(new_dense_acc) + epsilon)
    row_grads = clip * emb_grads
    square_mean = jnp.mean(row_grads * row_grads, axis=1)
    updated_acc = row_acc[touched] + square_mean
    new_row_acc = row_acc.at[touched].set(updated_acc)
    updated_rows = (
        table[touched] - learn_rate * row_grads / (jnp.sqrt(updated_acc) + epsilon)[:, None]
    )
    new_table = table.at[touched].set(updated_rows)
    return (new_dense, new_dense_acc, new_table, new_row_acc)


def solution(mesh):
    return jax.shard_map(
        body,
        mesh=mesh,
        in_specs=(
            P(("gx", "gy"), None, None),
            P(("gx", "gy"), None),
            P(("gx", "gy"), None),
            P(("gx", "gy"), None),
            P(("gx", "gy")),
            P(("gx", "gy")),
            P(("gx", "gy"), None),
        ),
        out_specs=(
            P(("gx", "gy"), None),
            P(("gx", "gy"), None),
            P(("gx", "gy"), None),
            P(("gx", "gy")),
        ),
        check_vma=False,
    )
```

```python
import functools

import jax
import jax.numpy as jnp
from jax import lax
from jax.experimental import pallas as pl
from jax.experimental.pallas import tpu as pltpu
from jax.sharding import PartitionSpec as P

learn_rate = 0.5
max_norm = 8.0
epsilon = 1e-10

MESH = pl.DeviceIdType.MESH
NX, NZ, NY, NC = 4, 8, 4, 2
SHARDS = 256
XS, YS, ZS = 3, 3, 2
UNITS = XS + YS + ZS
LANES = 128
F32 = jnp.float32


class Sends:
    def __init__(self, send_sems, recv_sems):
        self.send_sems, self.recv_sems = send_sems, recv_sems
        self.made = {}

    def start(self, name, src, dst, device):
        slot = len(self.made)
        copy = pltpu.make_async_remote_copy(
            src_ref=src,
            dst_ref=dst,
            send_sem=self.send_sems.at[slot],
            recv_sem=self.recv_sems.at[slot],
            device_id=device,
            device_id_type=MESH,
        )
        copy.start()
        self.made[name] = copy

    def wait(self, name):
        self.made[name].wait_recv()

    def drain(self):
        for copy in self.made.values():
            copy.wait_send()


def reduce_kernel(
    g_ref, e_ref, table_ref, row_acc_ref, touched_ref,
    mean_ref, norm_ref, tab, emb, row_tab, row_sq, row_ra, flat_sq,
    acc, pair, idx, ra,
    a_relay, a_last, a_mid, a_end,
    b_relay, b_last, b_mid, b_end,
    c_far, c_chain, c_mid, c_end,
    n_own, n_one, n_sum, n_two,
    send_sems, recv_sems, load_sems,
):
    gx, gy = lax.axis_index("gx"), lax.axis_index("gy")
    x, z = gx // NZ, gx % NZ
    y, c = gy // NC, gy % NC

    def dev(dx=0, dy=0, dz=0, core=None):
        return (
            ((x + dx) % NX) * NZ + (z + dz) % NZ,
            ((y + dy) % NY) * NC + (c if core is None else core),
        )

    def dev_zc(k):
        q = (z * NC + c + k) % (NZ * NC)
        return (x * NZ + q // NC, y * NC + q % NC)

    def dev_xy(k):
        q = (x * NY + y + k) % (NX * NY)
        return ((q // NY) * NZ + z, (q % NY) * NC + c)

    cols = lambda u: pl.ds(u * LANES, LANES)
    order = [0, 3, 6, 1, 4, 7, 2, 5]
    loads = {}
    for u in order:
        loads[u] = pltpu.make_async_copy(
            g_ref.at[:, :, :, c, :, cols(u)], acc.at[u], load_sems.at[u]
        )
        loads[u].start()
    prep_loads = [
        pltpu.make_async_copy(src, dst, load_sems.at[UNITS + i])
        for i, (src, dst) in enumerate(
            ((e_ref, emb), (touched_ref, idx), (row_acc_ref, ra), (table_ref, tab))
        )
    ]
    for copy in prep_loads:
        copy.start()

    barrier = pltpu.get_barrier_semaphore()
    for k in range(1, 16):
        pl.semaphore_signal(barrier, inc=1, device_id=dev_zc(k), device_id_type=MESH)
        pl.semaphore_signal(barrier, inc=1, device_id=dev_xy(k), device_id_type=MESH)
    pl.semaphore_wait(barrier, 30)

    net = Sends(send_sems, recv_sems)
    other = 1 - c
    mate = dev(core=other)

    def part(ref, u, kind, k):
        if kind == "x":
            return ref.at[u, (x + k) % NX]
        if kind == "y":
            return ref.at[u, :, :, (y + k) % NY]
        return ref.at[u, :, (z + k) % NZ]

    def give(u, kind, k):
        if kind == "x":
            src = g_ref.at[(x + k) % NX, :, :, other, :, cols(u)]
        elif kind == "y":
            src = g_ref.at[:, :, (y + k) % NY, other, :, cols(u)]
        else:
            src = g_ref.at[:, (z + k) % NZ, :, other, :, cols(u)]
        net.start(("pair", u, k), src, part(pair, u, kind, k), mate)

    kinds = {u: "x" if u < XS else "y" if u < XS + YS else "z" for u in range(UNITS)}
    waves = [[0, 3, 6], [1, 4, 7], [2, 5]]
    far_of = {"x": [2], "y": [2], "z": [4]}
    near_of = {"x": [1, 3, 0], "y": [1, 3, 0], "z": [3, 5, 2, 6, 1, 7, 0]}
    for wave in waves:
        for u in wave:
            for k in far_of[kinds[u]]:
                give(u, kinds[u], k)
        for u in wave:
            for k in near_of[kinds[u]]:
                give(u, kinds[u], k)

    def take(u, k):
        kind = kinds[u]
        net.wait(("pair", u, k))
        mine = part(acc, u, kind, k)
        mine[...] = mine[...] + part(pair, u, kind, k)[...]

    loaded = set()

    def load(u):
        if u not in loaded:
            loaded.add(u)
            loads[u].wait()

    LO, HI = pl.ds(0, 4), pl.ds(4, 4)

    def a_part(u, k, half):
        return acc.at[u, (x + k) % NX, half]

    def a_far(w):
        u = w
        load(u)
        take(u, 2)
        net.start(("ar", w), a_part(u, 2, LO), a_relay.at[w, 0], dev(dx=1))
        net.start(("al", w), a_part(u, 2, HI), a_relay.at[w, 1], dev(dx=-1))

    def a_near(w):
        u = w
        take(u, 1)
        net.start(("aer", w), a_part(u, 1, HI), a_last.at[w, 0, HI], dev(dx=1))
        take(u, 3)
        net.start(("ael", w), a_part(u, 3, LO), a_last.at[w, 1, LO], dev(dx=-1))
        take(u, 0)

    def a_late(w):
        u = w
        net.wait(("ar", w))
        ref = a_part(u, 1, LO)
        ref[...] = ref[...] + a_relay[w, 0]
        net.start(("alr", w), ref, a_last.at[w, 0, LO], dev(dx=1))
        net.wait(("al", w))
        ref = a_part(u, 3, HI)
        ref[...] = ref[...] + a_relay[w, 1]
        net.start(("all", w), ref, a_last.at[w, 1, HI], dev(dx=-1))

    def a_two(w):
        u = w
        for name in ("aer", "ael", "alr", "all"):
            net.wait((name, w))
        ref = acc.at[u, x]
        ref[...] = ref[...] + (a_last[w, 0] + a_last[w, 1])
        for k in (2, 1, 3):
            net.start(("am", w, k), acc.at[u, x, :, (y + k) % NY], a_mid.at[w, k - 1], dev(dy=k))

    def a_three(w):
        u = w
        for k in (1, 3, 2):
            net.wait(("am", w, k))
        ref = acc.at[u, x, :, y]
        ref[...] = ref[...] + (a_mid[w, 0] + a_mid[w, 1] + a_mid[w, 2])
        for k in (4, 3, 5, 2, 6, 1, 7):
            net.start(("ae", w, k), acc.at[u, x, (z + k) % NZ, y], a_end.at[w, k - 1], dev(dz=k))

    def b_part(u, k, half):
        return acc.at[u, :, half, (y + k) % NY]

    def b_far(w):
        u = XS + w
        load(u)
        take(u, 2)
        net.start(("br", w), b_part(u, 2, LO), b_relay.at[w, 0], dev(dy=1))
        net.start(("bl", w), b_part(u, 2, HI), b_relay.at[w, 1], dev(dy=-1))

    def b_near(w):
        u = XS + w
        take(u, 1)
        net.start(("ber", w), b_part(u, 1, HI), b_last.at[w, 0, :, HI], dev(dy=1))
        take(u, 3)
        net.start(("bel", w), b_part(u, 3, LO), b_last.at[w, 1, :, LO], dev(dy=-1))
        take(u, 0)

    def b_late(w):
        u = XS + w
        net.wait(("br", w))
        ref = b_part(u, 1, LO)
        ref[...] = ref[...] + b_relay[w, 0]
        net.start(("blr", w), ref, b_last.at[w, 0, :, LO], dev(dy=1))
        net.wait(("bl", w))
        ref = b_part(u, 3, HI)
        ref[...] = ref[...] + b_relay[w, 1]
        net.start(("bll", w), ref, b_last.at[w, 1, :, HI], dev(dy=-1))

    def b_two(w):
        u = XS + w
        for name in ("ber", "bel", "blr", "bll"):
            net.wait((name, w))
        ref = acc.at[u, :, :, y]
        ref[...] = ref[...] + (b_last[w, 0] + b_last[w, 1])
        for k in (2, 1, 3):
            net.start(("bm", w, k), acc.at[u, (x + k) % NX, :, y], b_mid.at[w, k - 1], dev(dx=k))

    def b_three(w):
        u = XS + w
        for k in (1, 3, 2):
            net.wait(("bm", w, k))
        ref = acc.at[u, x, :, y]
        ref[...] = ref[...] + (b_mid[w, 0] + b_mid[w, 1] + b_mid[w, 2])
        for k in (4, 3, 5, 2, 6, 1, 7):
            net.start(("be", w, k), acc.at[u, x, (z + k) % NZ, y], b_end.at[w, k - 1], dev(dz=k))

    XLO, XHI = pl.ds(0, 2), pl.ds(2, 2)

    def c_part(u, k, half=slice(None)):
        return acc.at[u, half, (z + k) % NZ]

    def c_zero(w):
        u = XS + YS + w
        load(u)
        take(u, 4)
        net.start(("c1r", w), c_part(u, 4, XLO), c_far.at[w, 0], dev(dz=1))
        net.start(("c1l", w), c_part(u, 4, XHI), c_far.at[w, 1], dev(dz=-1))

    def c_near(w):
        u = XS + YS + w
        take(u, 3)
        net.start(("c2er", w), c_part(u, 3, XHI), c_chain.at[w, 0, 0, XHI], dev(dz=1))
        take(u, 5)
        net.start(("c2el", w), c_part(u, 5, XLO), c_chain.at[w, 1, 0, XLO], dev(dz=-1))
        for k in (2, 6, 1, 7, 0):
            take(u, k)

    def c_one(w):
        u = XS + YS + w
        net.wait(("c1r", w))
        ref = c_part(u, 3, XLO)
        ref[...] = ref[...] + c_far[w, 0]
        net.start(("c2lr", w), ref, c_chain.at[w, 0, 0, XLO], dev(dz=1))
        net.wait(("c1l", w))
        ref = c_part(u, 5, XHI)
        ref[...] = ref[...] + c_far[w, 1]
        net.start(("c2ll", w), ref, c_chain.at[w, 1, 0, XHI], dev(dz=-1))

    def c_two(w):
        u = XS + YS + w
        net.wait(("c2er", w))
        net.wait(("c2lr", w))
        ref = c_part(u, 2)
        ref[...] = ref[...] + c_chain[w, 0, 0]
        net.start(("c3r", w), ref, c_chain.at[w, 0, 1], dev(dz=1))
        net.wait(("c2el", w))
        net.wait(("c2ll", w))
        ref = c_part(u, 6)
        ref[...] = ref[...] + c_chain[w, 1, 0]
        net.start(("c3l", w), ref, c_chain.at[w, 1, 1], dev(dz=-1))

    def c_three(w):
        u = XS + YS + w
        net.wait(("c3r", w))
        ref = c_part(u, 1)
        ref[...] = ref[...] + c_chain[w, 0, 1]
        net.start(("c4r", w), ref, c_chain.at[w, 0, 2], dev(dz=1))
        net.wait(("c3l", w))
        ref = c_part(u, 7)
        ref[...] = ref[...] + c_chain[w, 1, 1]
        net.start(("c4l", w), ref, c_chain.at[w, 1, 2], dev(dz=-1))

    def c_four(w):
        u = XS + YS + w
        net.wait(("c4r", w))
        net.wait(("c4l", w))
        ref = acc.at[u, :, z]
        ref[...] = ref[...] + (c_chain[w, 0, 2] + c_chain[w, 1, 2])
        for k in (2, 1, 3):
            net.start(("cm", w, k), acc.at[u, (x + k) % NX, z], c_mid.at[w, k - 1], dev(dx=k))

    def c_five(w):
        u = XS + YS + w
        for k in (1, 3, 2):
            net.wait(("cm", w, k))
        ref = acc.at[u, x, z]
        ref[...] = ref[...] + (c_mid[w, 0] + c_mid[w, 1] + c_mid[w, 2])
        for k in (2, 1, 3):
            net.start(("ce", w, k), acc.at[u, x, z, (y + k) % NY], c_end.at[w, k - 1], dev(dy=k))

    squares = []

    def prep_start():
        for copy in prep_loads:
            copy.wait()
        grads = emb[...]
        own = grads * grads
        squares.append(jnp.sum(own.reshape(-1, 8, LANES), axis=0))
        mean = jnp.sum(own, axis=1, keepdims=True) / F32(LANES)
        row_sq[...] = jnp.broadcast_to(mean, row_sq.shape)

    spot = lax.broadcasted_iota(jnp.int32, (32, LANES), 0) * LANES
    spot = spot + lax.broadcasted_iota(jnp.int32, (32, LANES), 1)
    flat = [jnp.zeros((32, LANES), F32)]

    def prep(part, parts=8):
        size = 512 // parts

        def eight(i, total):
            base = part * size + i * 8
            for j in range(8):
                t = base + j
                r = idx[t]
                row_tab[pl.ds(t, 1), :] = tab[pl.ds(r, 1), :]
                row_ra[pl.ds(t, 1), :] = jnp.full((1, LANES), ra[r], F32)
                total = jnp.where(spot == r, row_sq[pl.ds(t, 1), :], total)
            return total

        flat[0] = lax.fori_loop(0, size // 8, eight, flat[0])

    def end(u, name, w, ends, ks):
        total = acc[u, x, z, y]
        for k in ks:
            net.wait((name, w, k))
            total = total + ends[w, k - 1]
        mean = total / F32(SHARDS)
        mean_ref[:, cols(u)] = mean
        squares.append(mean * mean)

    def a_end_step(w):
        end(w, "ae", w, a_end, (1, 7, 2, 6, 3, 5, 4))

    def b_end_step(w):
        end(XS + w, "be", w, b_end, (1, 7, 2, 6, 3, 5, 4))

    def c_end_step(w):
        end(XS + YS + w, "ce", w, c_end, (1, 3, 2))

    a_far(0); b_far(0); c_zero(0)
    a_near(0); b_near(0); c_near(0)
    a_far(1); b_far(1); c_zero(1)
    c_one(0); a_late(0); b_late(0)
    a_near(1); b_near(1); c_near(1)
    a_far(2); b_far(2)
    prep_start()
    c_two(0)
    c_one(1)
    a_late(1); b_late(1)
    a_near(2); b_near(2)
    prep(0)
    a_two(0); b_two(0)
    prep(1)
    c_three(0); c_two(1)
    a_late(2); b_late(2)
    a_two(1); b_two(1)
    prep(2)
    a_three(0); b_three(0)
    prep(3)
    c_four(0); c_three(1)
    a_three(1); b_three(1)
    prep(4)
    a_end_step(0); b_end_step(0)
    a_two(2); b_two(2)
    c_five(0); c_four(1)
    prep(5)
    c_end_step(0)
    prep(6)
    a_end_step(1); b_end_step(1)
    a_three(2); b_three(2)
    c_five(1)
    prep(7)
    flat_sq[...] = flat[0]
    c_end_step(1)
    a_end_step(2); b_end_step(2)

    total = functools.reduce(lambda p, q: p + q, squares)
    n_own[...] = jnp.sum(total, axis=0, keepdims=True)
    for k in range(1, 16):
        net.start(("n1", k), n_own, n_one.at[k - 1], dev_zc(k))
    line = n_own[...]
    for k in range(1, 16):
        net.wait(("n1", k))
    for k in range(1, 16):
        line = line + n_one[k - 1]
    n_sum[...] = line
    for k in range(1, 16):
        net.start(("n2", k), n_sum, n_two.at[k - 1], dev_xy(k))
    for k in range(1, 16):
        net.wait(("n2", k))
    for k in range(1, 16):
        line = line + n_two[k - 1]
    norm_ref[...] = line
    net.drain()


def reduce_mean(grads, emb, table, row_acc, touched):
    vm = lambda *shape: pltpu.VMEM(shape + (8, LANES), F32)
    row = lambda *shape: pltpu.VMEM(shape + (1, LANES), F32)
    copies = 4 * (XS + YS) + 8 * ZS + 16 * (XS + YS) + 16 * ZS + 30
    shapes = ((8, 1024), (1, LANES), table.shape) + (emb.shape,) * 4 + ((32, LANES),)
    return pl.pallas_call(
        reduce_kernel,
        name="reduce_mean",
        out_shape=[jax.ShapeDtypeStruct(shape, F32) for shape in shapes],
        in_specs=[pl.BlockSpec(memory_space=pltpu.HBM)] * 5,
        out_specs=[pl.BlockSpec(memory_space=pltpu.VMEM)] * len(shapes),
        scratch_shapes=[
            vm(UNITS, NX, NZ, NY),
            vm(UNITS, NX, NZ, NY),
            pltpu.SMEM(touched.shape, jnp.int32),
            pltpu.SMEM(row_acc.shape, F32),
            vm(XS, 2, 4, NY), vm(XS, 2, NZ, NY), vm(XS, 3, NZ), vm(XS, 7),
            vm(YS, 2, NX, 4), vm(YS, 2, NX, NZ), vm(YS, 3, NZ), vm(YS, 7),
            vm(ZS, 2, 2, NY), vm(ZS, 2, 3, NX, NY), vm(ZS, 3, NY), vm(ZS, 3),
            row(), row(15), row(), row(15),
            pltpu.SemaphoreType.DMA((copies,)),
            pltpu.SemaphoreType.DMA((copies,)),
            pltpu.SemaphoreType.DMA((UNITS + 4,)),
        ],
        compiler_params=pltpu.CompilerParams(
            collective_id=0, has_side_effects=True, vmem_limit_bytes=50 * 1024 * 1024
        ),
    )(grads.reshape(NX, NZ, NY, NC, 8, 1024), emb, table, row_acc, touched)


def update_kernel(
    norm_ref, mean_ref, tab_ref, emb_ref, row_tab, row_sq, row_ra, flat_sq,
    param_ref, acc_ref, ra_ref, touched_ref,
    dense_out, dense_acc_out, table_out, row_acc_out, tab,
    idx, rows, dense_new, dense_acc_new, ra_new, sems,
):
    load = pltpu.make_async_copy(touched_ref, idx, sems.at[0])
    load.start()
    norm_sq = jnp.sum(norm_ref[...], axis=1, keepdims=True)
    clip = jnp.minimum(F32(1.0), F32(max_norm) / (jnp.sqrt(norm_sq) + F32(1e-06)))
    square = clip * clip
    live = clip > 0.0

    def grown(old, mean_square):
        return old + jnp.where(live, square * mean_square, 0.0)

    new_ra = grown(row_ra[...], row_sq[...])
    step = (F32(learn_rate) * clip) * emb_ref[...] / (jnp.sqrt(new_ra) + F32(epsilon))
    rows[...] = row_tab[...] - step
    load.wait()

    def sixteen(i, carry):
        for j in range(16):
            t = i * 16 + j
            tab[pl.ds(idx[t], 1), :] = rows[pl.ds(t, 1), :]
        return carry

    lax.fori_loop(0, 32, sixteen, 0)
    out = [pltpu.make_async_copy(tab, table_out, sems.at[1])]
    out[0].start()
    ra_new[...] = grown(ra_ref[...], flat_sq[...])
    scaled = clip * mean_ref[...]
    grow = acc_ref[...] + scaled * scaled
    dense_acc_new[...] = grow
    dense_new[...] = param_ref[...] - F32(learn_rate) * scaled / (jnp.sqrt(grow) + F32(epsilon))
    for i, (src, dst) in enumerate(
        ((ra_new, row_acc_out), (dense_acc_new, dense_acc_out), (dense_new, dense_out))
    ):
        out.append(pltpu.make_async_copy(src, dst, sems.at[2 + i]))
        out[-1].start()
    for copy in out:
        copy.wait()


def body(dense_grads, dense_param, dense_acc, table, row_acc, touched, emb_grads):
    mean, norm, tab, emb, row_tab, row_sq, row_ra, flat_sq = reduce_mean(
        dense_grads, emb_grads, table, row_acc, touched
    )
    vmem, hbm = pl.BlockSpec(memory_space=pltpu.VMEM), pl.BlockSpec(memory_space=pltpu.HBM)
    shapes = (dense_param.shape, dense_param.shape, table.shape, (32, LANES), table.shape)
    new_dense, new_dense_acc, new_table, new_row_acc, _ = pl.pallas_call(
        update_kernel,
        name="update",
        out_shape=[jax.ShapeDtypeStruct(shape, F32) for shape in shapes],
        in_specs=[vmem] * 11 + [hbm],
        out_specs=[hbm] * 4 + [vmem],
        scratch_shapes=[
            pltpu.SMEM(touched.shape, jnp.int32),
            pltpu.VMEM(emb.shape, F32),
            pltpu.VMEM(dense_param.shape, F32),
            pltpu.VMEM(dense_param.shape, F32),
            pltpu.VMEM((32, LANES), F32),
            pltpu.SemaphoreType.DMA((5,)),
        ],
        input_output_aliases={2: 4},
        compiler_params=pltpu.CompilerParams(vmem_limit_bytes=16 * 1024 * 1024),
    )(
        norm, mean, tab, emb, row_tab, row_sq, row_ra, flat_sq,
        dense_param, dense_acc, row_acc.reshape(32, LANES), touched,
    )
    return (new_dense, new_dense_acc, new_table, new_row_acc.reshape(-1))


def solution(mesh):
    return jax.shard_map(
        body,
        mesh=mesh,
        in_specs=(
            P(("gx", "gy"), None, None),
            P(("gx", "gy"), None),
            P(("gx", "gy"), None),
            P(("gx", "gy"), None),
            P(("gx", "gy")),
            P(("gx", "gy")),
            P(("gx", "gy"), None),
        ),
        out_specs=(
            P(("gx", "gy"), None),
            P(("gx", "gy"), None),
            P(("gx", "gy"), None),
            P(("gx", "gy")),
        ),
        check_vma=False,
    )
```

```python
import functools

import jax
import jax.numpy as jnp
from jax import lax
from jax.experimental import pallas as pl
from jax.experimental.pallas import tpu as pltpu
from jax.sharding import PartitionSpec as P

learn_rate = 0.5
max_norm = 8.0
epsilon = 1e-10

MESH = pl.DeviceIdType.MESH
NX, NZ, NY, NC = 4, 8, 4, 2
SHARDS = 256
XS, YS, ZS = 3, 3, 2
UNITS = XS + YS + ZS
LANES = 128
SEMS = 88
F32 = jnp.float32


PLANE = sorted(
    [(dx, dy) for dx in range(NX) for dy in range(NY) if dx or dy],
    key=lambda d: -(min(d[0], NX - d[0]) + min(d[1], NY - d[1])),
)


def far(k):
    dx, dz, dy = k // (NZ * NY * NC), k // (NY * NC) % NZ, k // NC % NY
    return min(dx, NX - dx) + min(dz, NZ - dz) + min(dy, NY - dy)


RANKS = sorted(range(1, SHARDS), key=lambda k: -far(k))


class Net:
    def __init__(self, sems, mate):
        self.sems, self.mate = sems, mate
        self.slots, self.sent = {}, {}

    def sem(self, name):
        return self.sems.at[self.slots.setdefault(name, len(self.slots))]

    def start(self, name, whole, src, dst, device):
        self.sent[name[0]] = whole
        pltpu.make_async_remote_copy(
            src_ref=src,
            dst_ref=dst,
            send_sem=self.sem(("sent", name[0])),
            recv_sem=self.sem(name),
            device_id=device,
            device_id_type=MESH,
        ).start()

    def filled(self, ref, recv, sent):
        return pltpu.make_async_remote_copy(
            src_ref=ref,
            dst_ref=ref,
            send_sem=self.sem(sent),
            recv_sem=self.sem(recv),
            device_id=self.mate,
            device_id_type=MESH,
        )

    def wait(self, name, ref):
        self.filled(ref, name, ("sent", name[0])).wait_recv()

    def drain(self):
        for buffer, ref in self.sent.items():
            self.filled(ref, ("sent", buffer), ("sent", buffer)).wait_send()
        self.sent = {}


def reduce_kernel(
    g_ref, e_ref, table_ref, row_acc_ref, touched_ref,
    mean_ref, norm_ref, tab, emb, row_tab, row_sq, row_ra, flat_sq,
    acc, pair, idx, ra,
    a_relay, a_last, a_mid, a_end,
    b_relay, b_last, b_mid, b_end,
    c_far, c_chain, c_end,
    n_all,
    net_sems, load_sems,
):
    gx, gy = lax.axis_index("gx"), lax.axis_index("gy")
    x, z = gx // NZ, gx % NZ
    y, c = gy // NC, gy % NC

    def dev(dx=0, dy=0, dz=0, core=None):
        return (
            ((x + dx) % NX) * NZ + (z + dz) % NZ,
            ((y + dy) % NY) * NC + (c if core is None else core),
        )

    cols = lambda u: pl.ds(u * LANES, LANES)
    loads = {}
    for u in (0, 3, 6, 7, 1, 4, 2, 5):
        loads[u] = pltpu.make_async_copy(
            g_ref.at[:, :, :, c, :, cols(u)], acc.at[u], load_sems.at[u]
        )
        loads[u].start()
    prep_loads = [
        pltpu.make_async_copy(src, dst, load_sems.at[UNITS + i])
        for i, (src, dst) in enumerate(
            ((e_ref, emb), (touched_ref, idx), (row_acc_ref, ra), (table_ref, tab))
        )
    ]
    for copy in prep_loads:
        copy.start()

    barrier = pltpu.get_barrier_semaphore()
    nearby = [dev(core=1 - c)] + [dev(**{axis: step}) for axis in ("dx", "dy", "dz") for step in (1, -1)]
    for device in nearby:
        pl.semaphore_signal(barrier, inc=1, device_id=device, device_id_type=MESH)
    pl.semaphore_wait(barrier, len(nearby))

    other = 1 - c
    mate = dev(core=other)
    net = Net(net_sems, mate)
    kinds = {u: "x" if u < XS else "y" if u < XS + YS else "z" for u in range(UNITS)}

    def part(ref, u, k):
        if kinds[u] == "x":
            return ref.at[u, (x + k) % NX]
        if kinds[u] == "y":
            return ref.at[u, :, :, (y + k) % NY]
        return ref.at[u, :, (z + k) % NZ]

    def give(u, ks):
        for k in ks:
            if kinds[u] == "x":
                src = g_ref.at[(x + k) % NX, :, :, other, :, cols(u)]
            elif kinds[u] == "y":
                src = g_ref.at[:, :, (y + k) % NY, other, :, cols(u)]
            else:
                src = g_ref.at[:, (z + k) % NZ, :, other, :, cols(u)]
            net.start(("pair", u, ks), pair, src, part(pair, u, k), mate)

    loaded = set()

    def take(u, ks):
        if u not in loaded:
            loaded.add(u)
            loads[u].wait()
        if kinds[u] == "x":
            span = pair.at[u, pl.ds(0, len(ks))]
        elif kinds[u] == "y":
            span = pair.at[u, :, :, pl.ds(0, len(ks))]
        else:
            span = pair.at[u, :, pl.ds(0, len(ks))]
        net.wait(("pair", u, ks), span)
        for k in ks:
            mine = part(acc, u, k)
            mine[...] = mine[...] + part(pair, u, k)[...]

    FAR, NEAR, OWN = (2,), (1, 3), (0,)
    C1, C2, C3, C4 = (4,), (3, 5), (2, 6), (1, 7, 0)
    for us, ks in (
        ((0, 3), FAR), ((6, 7), C1), ((0, 3), NEAR), ((6, 7), C2), ((1, 4), FAR), ((6, 7), C3),
        ((1, 4), NEAR), ((2, 5), FAR), ((6, 7), C4), ((0, 3), OWN), ((2, 5), NEAR), ((1, 4, 2, 5), OWN),
    ):
        for u in us:
            give(u, ks)

    LO, HI = pl.ds(0, 4), pl.ds(4, 4)

    def tree(tag, axis, relay, last, view, mine):
        def far(w):
            net.start((tag + "r", w, 0), relay, view(w, 2, LO), relay.at[w, 0], dev(**{axis: 1}))
            net.start((tag + "r", w, 1), relay, view(w, 2, HI), relay.at[w, 1], dev(**{axis: -1}))

        def land(w, side, half):
            return last.at[w, side, half] if axis == "dx" else last.at[w, side, :, half]

        def near(w):
            net.start((tag + "l", w), last, view(w, 1, HI), land(w, 0, HI), dev(**{axis: 1}))
            net.start((tag + "l", w), last, view(w, 3, LO), land(w, 1, LO), dev(**{axis: -1}))

        def late(w):
            for side, k, half in ((0, 1, LO), (1, 3, HI)):
                net.wait((tag + "r", w, side), relay.at[w, side])
                ref = view(w, k, half)
                ref[...] = ref[...] + relay[w, side]
                net.start((tag + "l", w), last, ref, land(w, side, half), dev(**{axis: 1 - 2 * side}))

        def final(w):
            net.wait((tag + "l", w), last.at[w])
            ref = mine(w)
            ref[...] = ref[...] + (last[w, 0] + last[w, 1])

        return far, near, late, final

    a_steps = tree(
        "a", "dx", a_relay, a_last,
        lambda w, k, half: acc.at[w, (x + k) % NX, half],
        lambda w: acc.at[w, x],
    )

    def a_far(w):
        take(w, FAR)
        a_steps[0](w)

    def a_near(w):
        take(w, NEAR)
        a_steps[1](w)

    def a_late(w):
        a_steps[2](w)

    def a_two(w):
        take(w, OWN)
        a_steps[3](w)
        for k in (2, 1, 3):
            net.start(("am", w), a_mid, acc.at[w, x, :, (y + k) % NY], a_mid.at[w, k - 1], dev(dy=k))

    def line(tag, w, u, mid, ends):
        net.wait((tag + "m", w), mid.at[w])
        ref = acc.at[u, x, :, y]
        ref[...] = ref[...] + (mid[w, 0] + mid[w, 1] + mid[w, 2])
        for k in (4, 3, 5, 2, 6, 1, 7):
            net.start((tag + "e", w), ends, acc.at[u, x, (z + k) % NZ, y], ends.at[w, k - 1], dev(dz=k))

    def a_three(w):
        line("a", w, w, a_mid, a_end)

    b_steps = tree(
        "b", "dy", b_relay, b_last,
        lambda w, k, half: acc.at[XS + w, :, half, (y + k) % NY],
        lambda w: acc.at[XS + w, :, :, y],
    )

    def b_far(w):
        take(XS + w, FAR)
        b_steps[0](w)

    def b_near(w):
        take(XS + w, NEAR)
        b_steps[1](w)

    def b_late(w):
        b_steps[2](w)

    def b_two(w):
        take(XS + w, OWN)
        b_steps[3](w)
        for k in (2, 1, 3):
            net.start(("bm", w), b_mid, acc.at[XS + w, (x + k) % NX, :, y], b_mid.at[w, k - 1], dev(dx=k))

    def b_three(w):
        line("b", w, XS + w, b_mid, b_end)

    XLO, XHI = pl.ds(0, 2), pl.ds(2, 2)

    def c_part(w, k, half=slice(None)):
        return acc.at[XS + YS + w, half, (z + k) % NZ]

    def c_zero(w):
        take(XS + YS + w, C1)
        net.start(("cf", w, 0), c_far, c_part(w, 4, XLO), c_far.at[w, 0], dev(dz=1))
        net.start(("cf", w, 1), c_far, c_part(w, 4, XHI), c_far.at[w, 1], dev(dz=-1))

    def c_near(w):
        take(XS + YS + w, C2)
        net.start(("cc", w, 0, 0), c_chain, c_part(w, 3, XHI), c_chain.at[w, 0, 0, XHI], dev(dz=1))
        net.start(("cc", w, 1, 0), c_chain, c_part(w, 5, XLO), c_chain.at[w, 1, 0, XLO], dev(dz=-1))

    def c_one(w):
        for side, k, half in ((0, 3, XLO), (1, 5, XHI)):
            net.wait(("cf", w, side), c_far.at[w, side])
            ref = c_part(w, k, half)
            ref[...] = ref[...] + c_far[w, side]
            net.start(("cc", w, side, 0), c_chain, ref, c_chain.at[w, side, 0, half], dev(dz=1 - 2 * side))

    def c_pass(w, step, ks):
        for side, k in enumerate(ks):
            net.wait(("cc", w, side, step), c_chain.at[w, side, step])
            ref = c_part(w, k)
            ref[...] = ref[...] + c_chain[w, side, step]
            net.start(
                ("cc", w, side, step + 1), c_chain, ref, c_chain.at[w, side, step + 1], dev(dz=1 - 2 * side)
            )

    def c_two(w):
        take(XS + YS + w, C3)
        c_pass(w, 0, (2, 6))

    def c_three(w):
        take(XS + YS + w, C4)
        c_pass(w, 1, (1, 7))

    def c_four(w):
        for side in (0, 1):
            net.wait(("cc", w, side, 2), c_chain.at[w, side, 2])
        ref = c_part(w, 0)
        ref[...] = ref[...] + (c_chain[w, 0, 2] + c_chain[w, 1, 2])
        for dx, dy in PLANE:
            net.start(
                ("ce", w), c_end,
                acc.at[XS + YS + w, (x + dx) % NX, z, (y + dy) % NY],
                c_end.at[w, dx * NY + dy - 1],
                dev(dx=dx, dy=dy),
            )

    squares = []

    def prep_start():
        for copy in prep_loads:
            copy.wait()
        grads = emb[...]
        own = grads * grads
        squares.append(jnp.sum(own.reshape(-1, 8, LANES), axis=0))
        mean = jnp.sum(own, axis=1, keepdims=True) / F32(LANES)
        row_sq[...] = jnp.broadcast_to(mean, row_sq.shape)

    spot = lax.broadcasted_iota(jnp.int32, (32, LANES), 0) * LANES
    spot = spot + lax.broadcasted_iota(jnp.int32, (32, LANES), 1)
    flat = [jnp.zeros((32, LANES), F32)]

    def prep(part, parts=8):
        size = 512 // parts

        def eight(i, total):
            base = part * size + i * 8
            for j in range(8):
                t = base + j
                r = idx[t]
                row_tab[pl.ds(t, 1), :] = tab[pl.ds(r, 1), :]
                row_ra[pl.ds(t, 1), :] = jnp.full((1, LANES), ra[r], F32)
                total = jnp.where(spot == r, row_sq[pl.ds(t, 1), :], total)
            return total

        flat[0] = lax.fori_loop(0, size // 8, eight, flat[0])

    def end(u, name, w, ends):
        net.wait((name, w), ends.at[w])
        mean = (acc[u, x, z, y] + jnp.sum(ends[w], axis=0)) / F32(SHARDS)
        mean_ref[:, cols(u)] = mean
        squares.append(mean * mean)

    def a_end_step(w):
        end(w, "ae", w, a_end)

    def b_end_step(w):
        end(XS + w, "be", w, b_end)

    def c_end_step(w):
        end(XS + YS + w, "ce", w, c_end)

    a_far(0); b_far(0); c_zero(0); c_zero(1)
    a_near(0); b_near(0); c_near(0); c_near(1)
    a_far(1); b_far(1)
    c_one(0); a_late(0); b_late(0); c_one(1)
    a_near(1); b_near(1)
    a_far(2); b_far(2)
    prep_start()
    c_two(0)
    a_late(1); b_late(1)
    c_two(1)
    a_near(2); b_near(2)
    prep(0)
    prep(1)
    c_three(0); c_three(1)
    prep(2)
    a_late(2); b_late(2)
    a_two(0); b_two(0)
    prep(3)
    a_two(1); b_two(1)
    prep(4)
    a_two(2); b_two(2)
    c_four(0); c_four(1)
    prep(5)
    prep(6)
    a_three(0); b_three(0)
    a_three(1); b_three(1)
    prep(7)
    flat_sq[...] = flat[0]
    a_three(2); b_three(2)
    c_end_step(0)
    c_end_step(1)
    a_end_step(0); b_end_step(0)
    a_end_step(1); b_end_step(1)
    a_end_step(2); b_end_step(2)

    total = functools.reduce(lambda p, q: p + q, squares)
    n_all[pl.ds(0, 1), :] = jnp.sum(total, axis=0, keepdims=True)
    me = gx * (NY * NC) + gy
    own = n_all.at[pl.ds(0, 1)]
    rest = n_all.at[pl.ds(1, SHARDS - 1)]
    for k in RANKS:
        q = (me + k) % SHARDS
        device = (q // (NY * NC), q % (NY * NC))
        net.start(("norm",), rest, own, n_all.at[pl.ds(k, 1)], device)
    net.wait(("norm",), rest)
    norm_ref[...] = jnp.sum(n_all[...], axis=0, keepdims=True)
    net.drain()
    assert len(net.slots) == SEMS, len(net.slots)


def reduce_mean(grads, emb, table, row_acc, touched):
    vm = lambda *shape: pltpu.VMEM(shape + (8, LANES), F32)
    shapes = ((8, 1024), (1, LANES), table.shape) + (emb.shape,) * 4 + ((32, LANES),)
    return pl.pallas_call(
        reduce_kernel,
        name="reduce_mean",
        out_shape=[jax.ShapeDtypeStruct(shape, F32) for shape in shapes],
        in_specs=[pl.BlockSpec(memory_space=pltpu.HBM)] * 5,
        out_specs=[pl.BlockSpec(memory_space=pltpu.VMEM)] * len(shapes),
        scratch_shapes=[
            vm(UNITS, NX, NZ, NY),
            vm(UNITS, NX, NZ, NY),
            pltpu.SMEM(touched.shape, jnp.int32),
            pltpu.SMEM(row_acc.shape, F32),
            vm(XS, 2, 4, NY), vm(XS, 2, NZ, NY), vm(XS, 3, NZ), vm(XS, 7),
            vm(YS, 2, NX, 4), vm(YS, 2, NX, NZ), vm(YS, 3, NZ), vm(YS, 7),
            vm(ZS, 2, 2, NY), vm(ZS, 2, 3, NX, NY), vm(ZS, NX * NY - 1),
            pltpu.VMEM((SHARDS, LANES), F32),
            pltpu.SemaphoreType.DMA((SEMS,)),
            pltpu.SemaphoreType.DMA((UNITS + 4,)),
        ],
        compiler_params=pltpu.CompilerParams(
            collective_id=0, has_side_effects=True, vmem_limit_bytes=32 * 1024 * 1024
        ),
    )(*(
        pltpu.with_memory_space_constraint(value, pltpu.HBM)
        for value in (grads.reshape(NX, NZ, NY, NC, 8, 1024), emb, table, row_acc, touched)
    ))


def update_kernel(
    norm_ref, mean_ref, tab_ref, emb_ref, row_tab, row_sq, row_ra, flat_sq,
    param_ref, acc_ref, ra_ref, touched_ref,
    dense_out, dense_acc_out, table_out, row_acc_out, tab,
    idx, rows, dense_new, dense_acc_new, ra_new, sems,
):
    load = pltpu.make_async_copy(touched_ref, idx, sems.at[0])
    load.start()
    norm_sq = jnp.sum(norm_ref[...], axis=1, keepdims=True)
    clip = jnp.minimum(F32(1.0), F32(max_norm) / (jnp.sqrt(norm_sq) + F32(1e-06)))
    square = clip * clip
    live = clip > 0.0

    def grown(old, mean_square):
        return old + jnp.where(live, square * mean_square, 0.0)

    new_ra = grown(row_ra[...], row_sq[...])
    step = (F32(learn_rate) * clip) * emb_ref[...] / (jnp.sqrt(new_ra) + F32(epsilon))
    rows[...] = row_tab[...] - step
    load.wait()

    def sixteen(i, carry):
        for j in range(16):
            t = i * 16 + j
            tab[pl.ds(idx[t], 1), :] = rows[pl.ds(t, 1), :]
        return carry

    lax.fori_loop(0, 32, sixteen, 0)
    out = [pltpu.make_async_copy(tab, table_out, sems.at[1])]
    out[0].start()
    ra_new[...] = grown(ra_ref[...], flat_sq[...])
    scaled = clip * mean_ref[...]
    grow = acc_ref[...] + scaled * scaled
    dense_acc_new[...] = grow
    dense_new[...] = param_ref[...] - F32(learn_rate) * scaled / (jnp.sqrt(grow) + F32(epsilon))
    for i, (src, dst) in enumerate(
        ((ra_new, row_acc_out), (dense_acc_new, dense_acc_out), (dense_new, dense_out))
    ):
        out.append(pltpu.make_async_copy(src, dst, sems.at[2 + i]))
        out[-1].start()
    for copy in out:
        copy.wait()


def body(dense_grads, dense_param, dense_acc, table, row_acc, touched, emb_grads):
    mean, norm, tab, emb, row_tab, row_sq, row_ra, flat_sq = reduce_mean(
        dense_grads, emb_grads, table, row_acc, touched
    )
    vmem, hbm = pl.BlockSpec(memory_space=pltpu.VMEM), pl.BlockSpec(memory_space=pltpu.HBM)
    shapes = (dense_param.shape, dense_param.shape, table.shape, (32, LANES), table.shape)
    new_dense, new_dense_acc, new_table, new_row_acc, _ = pl.pallas_call(
        update_kernel,
        name="update",
        out_shape=[jax.ShapeDtypeStruct(shape, F32) for shape in shapes],
        in_specs=[vmem] * 11 + [hbm],
        out_specs=[hbm] * 4 + [vmem],
        scratch_shapes=[
            pltpu.SMEM(touched.shape, jnp.int32),
            pltpu.VMEM(emb.shape, F32),
            pltpu.VMEM(dense_param.shape, F32),
            pltpu.VMEM(dense_param.shape, F32),
            pltpu.VMEM((32, LANES), F32),
            pltpu.SemaphoreType.DMA((5,)),
        ],
        input_output_aliases={2: 4},
        compiler_params=pltpu.CompilerParams(vmem_limit_bytes=16 * 1024 * 1024),
    )(
        norm, mean, tab, emb, row_tab, row_sq, row_ra, flat_sq,
        dense_param, dense_acc, row_acc.reshape(32, LANES), touched,
    )
    return (new_dense, new_dense_acc, new_table, new_row_acc.reshape(-1))


def solution(mesh):
    return jax.shard_map(
        body,
        mesh=mesh,
        in_specs=(
            P(("gx", "gy"), None, None),
            P(("gx", "gy"), None),
            P(("gx", "gy"), None),
            P(("gx", "gy"), None),
            P(("gx", "gy")),
            P(("gx", "gy")),
            P(("gx", "gy"), None),
        ),
        out_specs=(
            P(("gx", "gy"), None),
            P(("gx", "gy"), None),
            P(("gx", "gy"), None),
            P(("gx", "gy")),
        ),
        check_vma=False,
    )
```

```python
import functools

import jax
import jax.numpy as jnp
from jax import lax
from jax.experimental import pallas as pl
from jax.experimental.pallas import tpu as pltpu
from jax.sharding import PartitionSpec as P

learn_rate = 0.5
max_norm = 8.0
epsilon = 1e-10

LOGICAL = pl.DeviceIdType.LOGICAL
NX, NZ, NY, NC = 4, 8, 4, 2
SHARDS = 256
XS, YS, ZS = 3, 3, 2
UNITS = XS + YS + ZS
LANES = 128
SEMS = 88
F32 = jnp.float32


PLANE = sorted(
    [(dx, dy) for dx in range(NX) for dy in range(NY) if dx or dy],
    key=lambda d: -(min(d[0], NX - d[0]) + min(d[1], NY - d[1])),
)


def hops(dx, dy, dz):
    return min(dx, NX - dx) + min(dy, NY - dy) + min(dz, NZ - dz)


ALL = sorted(
    [
        (dx, dz, dy, dc)
        for dx in range(NX) for dz in range(NZ) for dy in range(NY) for dc in range(NC)
        if dx or dz or dy or dc
    ],
    key=lambda d: -hops(d[0], d[2], d[1]),
)


class Net:
    def __init__(self, sems, mate):
        self.sems, self.mate = sems, mate
        self.slots, self.sent = {}, {}

    def sem(self, name):
        return self.sems.at[self.slots.setdefault(name, len(self.slots))]

    def start(self, name, whole, src, dst, device):
        self.sent[name[0]] = whole
        pltpu.make_async_remote_copy(
            src_ref=src,
            dst_ref=dst,
            send_sem=self.sem(("sent", name[0])),
            recv_sem=self.sem(name),
            device_id=device,
            device_id_type=LOGICAL,
        ).start()

    def filled(self, ref, recv, sent):
        return pltpu.make_async_remote_copy(
            src_ref=ref,
            dst_ref=ref,
            send_sem=self.sem(sent),
            recv_sem=self.sem(recv),
            device_id=self.mate,
            device_id_type=LOGICAL,
        )

    def wait(self, name, ref):
        self.filled(ref, name, ("sent", name[0])).wait_recv()

    def drain(self):
        for buffer, ref in self.sent.items():
            self.filled(ref, ("sent", buffer), ("sent", buffer)).wait_send()
        self.sent = {}


def reduce_kernel(
    g_ref, e_ref, table_ref, row_acc_ref, touched_ref,
    mean_ref, norm_ref, tab, emb, row_tab, row_sq, row_ra, flat_sq,
    acc, pair, idx, ra,
    a_relay, a_last, a_mid, a_end,
    b_relay, b_last, b_mid, b_end,
    c_far, c_chain, c_end,
    n_all,
    net_sems, load_sems,
):
    gx, gy = lax.axis_index("gx"), lax.axis_index("gy")
    x, z = lax.div(gx, NZ), lax.rem(gx, NZ)
    y, c = lax.div(gy, NC), lax.rem(gy, NC)
    at_x = [x] + [lax.rem(x + d, NX) for d in range(1, NX)]
    at_y = [y] + [lax.rem(y + d, NY) for d in range(1, NY)]
    at_z = [z] + [lax.rem(z + d, NZ) for d in range(1, NZ)]
    at_c = [c, 1 - c]
    base_x = [v * (NZ * NY * NC) for v in at_x]
    base_z = [v * (NY * NC) for v in at_z]
    base_y = [v * NC for v in at_y]

    def dev(dx=0, dy=0, dz=0, dc=0):
        return base_x[dx % NX] + base_z[dz % NZ] + (base_y[dy % NY] + at_c[dc])

    cols = lambda u: pl.ds(u * LANES, LANES)
    loads = {}
    for u in (0, 3, 6, 7, 1, 4, 2, 5):
        loads[u] = pltpu.make_async_copy(
            g_ref.at[:, :, :, c, :, cols(u)], acc.at[u], load_sems.at[u]
        )
        loads[u].start()
    prep_loads = [
        pltpu.make_async_copy(src, dst, load_sems.at[UNITS + i])
        for i, (src, dst) in enumerate(
            ((e_ref, emb), (touched_ref, idx), (row_acc_ref, ra), (table_ref, tab))
        )
    ]
    for copy in prep_loads:
        copy.start()

    barrier = pltpu.get_barrier_semaphore()
    nearby = [dev(dc=1)] + [dev(**{axis: step}) for axis in ("dx", "dy", "dz") for step in (1, -1)]
    for device in nearby:
        pl.semaphore_signal(barrier, inc=1, device_id=device, device_id_type=LOGICAL)
    pl.semaphore_wait(barrier, len(nearby))

    other = at_c[1]
    mate = dev(dc=1)
    net = Net(net_sems, mate)
    kinds = {u: "x" if u < XS else "y" if u < XS + YS else "z" for u in range(UNITS)}

    def part(ref, u, k):
        if kinds[u] == "x":
            return ref.at[u, at_x[k]]
        if kinds[u] == "y":
            return ref.at[u, :, :, at_y[k]]
        return ref.at[u, :, at_z[k]]

    def give(u, ks):
        for k in ks:
            if kinds[u] == "x":
                src = g_ref.at[at_x[k], :, :, other, :, cols(u)]
            elif kinds[u] == "y":
                src = g_ref.at[:, :, at_y[k], other, :, cols(u)]
            else:
                src = g_ref.at[:, at_z[k], :, other, :, cols(u)]
            net.start(("pair", u, ks), pair, src, part(pair, u, k), mate)

    loaded = set()

    def take(u, ks):
        if u not in loaded:
            loaded.add(u)
            loads[u].wait()
        if kinds[u] == "x":
            span = pair.at[u, pl.ds(0, len(ks))]
        elif kinds[u] == "y":
            span = pair.at[u, :, :, pl.ds(0, len(ks))]
        else:
            span = pair.at[u, :, pl.ds(0, len(ks))]
        net.wait(("pair", u, ks), span)
        for k in ks:
            mine = part(acc, u, k)
            mine[...] = mine[...] + part(pair, u, k)[...]

    FAR, NEAR, OWN = (2,), (1, 3), (0,)
    C1, C2, C3, C4 = (4,), (3, 5), (2, 6), (1, 7, 0)
    for us, ks in (
        ((0, 3), FAR), ((6, 7), C1), ((0, 3), NEAR), ((6, 7), C2), ((1, 4), FAR), ((6, 7), C3),
        ((1, 4), NEAR), ((2, 5), FAR), ((6, 7), C4), ((0, 3), OWN), ((2, 5), NEAR), ((1, 4, 2, 5), OWN),
    ):
        for u in us:
            give(u, ks)

    LO, HI = pl.ds(0, 4), pl.ds(4, 4)

    def tree(tag, axis, relay, last, view, mine):
        def far(w):
            net.start((tag + "r", w, 0), relay, view(w, 2, LO), relay.at[w, 0], dev(**{axis: 1}))
            net.start((tag + "r", w, 1), relay, view(w, 2, HI), relay.at[w, 1], dev(**{axis: -1}))

        def land(w, side, half):
            return last.at[w, side, half] if axis == "dx" else last.at[w, side, :, half]

        def near(w):
            net.start((tag + "l", w), last, view(w, 1, HI), land(w, 0, HI), dev(**{axis: 1}))
            net.start((tag + "l", w), last, view(w, 3, LO), land(w, 1, LO), dev(**{axis: -1}))

        def late(w):
            for side, k, half in ((0, 1, LO), (1, 3, HI)):
                net.wait((tag + "r", w, side), relay.at[w, side])
                ref = view(w, k, half)
                ref[...] = ref[...] + relay[w, side]
                net.start((tag + "l", w), last, ref, land(w, side, half), dev(**{axis: 1 - 2 * side}))

        def final(w):
            net.wait((tag + "l", w), last.at[w])
            ref = mine(w)
            ref[...] = ref[...] + (last[w, 0] + last[w, 1])

        return far, near, late, final

    a_steps = tree(
        "a", "dx", a_relay, a_last,
        lambda w, k, half: acc.at[w, at_x[k], half],
        lambda w: acc.at[w, x],
    )

    def a_far(w):
        take(w, FAR)
        a_steps[0](w)

    def a_near(w):
        take(w, NEAR)
        a_steps[1](w)

    def a_late(w):
        a_steps[2](w)

    def a_two(w):
        take(w, OWN)
        a_steps[3](w)
        for k in (2, 1, 3):
            net.start(("am", w), a_mid, acc.at[w, x, :, at_y[k]], a_mid.at[w, k - 1], dev(dy=k))

    def line(tag, w, u, mid, ends):
        net.wait((tag + "m", w), mid.at[w])
        ref = acc.at[u, x, :, y]
        ref[...] = ref[...] + (mid[w, 0] + mid[w, 1] + mid[w, 2])
        for k in (4, 3, 5, 2, 6, 1, 7):
            net.start((tag + "e", w), ends, acc.at[u, x, at_z[k], y], ends.at[w, k - 1], dev(dz=k))

    def a_three(w):
        line("a", w, w, a_mid, a_end)

    b_steps = tree(
        "b", "dy", b_relay, b_last,
        lambda w, k, half: acc.at[XS + w, :, half, at_y[k]],
        lambda w: acc.at[XS + w, :, :, y],
    )

    def b_far(w):
        take(XS + w, FAR)
        b_steps[0](w)

    def b_near(w):
        take(XS + w, NEAR)
        b_steps[1](w)

    def b_late(w):
        b_steps[2](w)

    def b_two(w):
        take(XS + w, OWN)
        b_steps[3](w)
        for k in (2, 1, 3):
            net.start(("bm", w), b_mid, acc.at[XS + w, at_x[k], :, y], b_mid.at[w, k - 1], dev(dx=k))

    def b_three(w):
        line("b", w, XS + w, b_mid, b_end)

    XLO, XHI = pl.ds(0, 2), pl.ds(2, 2)

    def c_part(w, k, half=slice(None)):
        return acc.at[XS + YS + w, half, at_z[k]]

    def c_zero(w):
        take(XS + YS + w, C1)
        net.start(("cf", w, 0), c_far, c_part(w, 4, XLO), c_far.at[w, 0], dev(dz=1))
        net.start(("cf", w, 1), c_far, c_part(w, 4, XHI), c_far.at[w, 1], dev(dz=-1))

    def c_near(w):
        take(XS + YS + w, C2)
        net.start(("cc", w, 0, 0), c_chain, c_part(w, 3, XHI), c_chain.at[w, 0, 0, XHI], dev(dz=1))
        net.start(("cc", w, 1, 0), c_chain, c_part(w, 5, XLO), c_chain.at[w, 1, 0, XLO], dev(dz=-1))

    def c_one(w):
        for side, k, half in ((0, 3, XLO), (1, 5, XHI)):
            net.wait(("cf", w, side), c_far.at[w, side])
            ref = c_part(w, k, half)
            ref[...] = ref[...] + c_far[w, side]
            net.start(("cc", w, side, 0), c_chain, ref, c_chain.at[w, side, 0, half], dev(dz=1 - 2 * side))

    def c_pass(w, step, ks):
        for side, k in enumerate(ks):
            net.wait(("cc", w, side, step), c_chain.at[w, side, step])
            ref = c_part(w, k)
            ref[...] = ref[...] + c_chain[w, side, step]
            net.start(
                ("cc", w, side, step + 1), c_chain, ref, c_chain.at[w, side, step + 1], dev(dz=1 - 2 * side)
            )

    def c_two(w):
        take(XS + YS + w, C3)
        c_pass(w, 0, (2, 6))

    def c_three(w):
        take(XS + YS + w, C4)
        c_pass(w, 1, (1, 7))

    def c_four(w):
        for side in (0, 1):
            net.wait(("cc", w, side, 2), c_chain.at[w, side, 2])
        ref = c_part(w, 0)
        ref[...] = ref[...] + (c_chain[w, 0, 2] + c_chain[w, 1, 2])
        for dx, dy in PLANE:
            net.start(
                ("ce", w), c_end,
                acc.at[XS + YS + w, at_x[dx], z, at_y[dy]],
                c_end.at[w, dx * NY + dy - 1],
                dev(dx=dx, dy=dy),
            )

    squares = []

    def prep_start():
        for copy in prep_loads:
            copy.wait()
        grads = emb[...]
        own = grads * grads
        squares.append(jnp.sum(own.reshape(-1, 8, LANES), axis=0))
        mean = jnp.sum(own, axis=1, keepdims=True) / F32(LANES)
        row_sq[...] = jnp.broadcast_to(mean, row_sq.shape)

    spot = lax.broadcasted_iota(jnp.int32, (32, LANES), 0) * LANES
    spot = spot + lax.broadcasted_iota(jnp.int32, (32, LANES), 1)
    flat = [jnp.zeros((32, LANES), F32)]

    def prep(part, parts=8):
        size = 512 // parts

        def eight(i, total):
            base = part * size + i * 8
            for j in range(8):
                t = base + j
                r = idx[t]
                row_tab[pl.ds(t, 1), :] = tab[pl.ds(r, 1), :]
                row_ra[pl.ds(t, 1), :] = jnp.full((1, LANES), ra[r], F32)
                total = jnp.where(spot == r, row_sq[pl.ds(t, 1), :], total)
            return total

        flat[0] = lax.fori_loop(0, size // 8, eight, flat[0])

    def end(u, name, w, ends):
        net.wait((name, w), ends.at[w])
        mean = (acc[u, x, z, y] + jnp.sum(ends[w], axis=0)) / F32(SHARDS)
        mean_ref[:, cols(u)] = mean
        squares.append(mean * mean)

    def a_end_step(w):
        end(w, "ae", w, a_end)

    def b_end_step(w):
        end(XS + w, "be", w, b_end)

    def c_end_step(w):
        end(XS + YS + w, "ce", w, c_end)

    a_far(0)
    b_far(0)
    c_zero(1)
    a_near(0)
    b_near(0)
    c_zero(0)
    c_near(0)
    b_far(1)
    a_far(1)
    a_near(1)
    c_near(1)
    a_late(0)
    c_one(1)
    b_late(0)
    a_far(2)
    c_one(0)
    b_far(2)
    b_near(1)
    b_late(1)
    a_late(1)
    c_two(1)
    a_near(2)
    b_near(2)
    c_two(0)
    b_late(2)
    a_two(0)
    a_late(2)
    b_two(0)
    a_two(1)
    c_three(1)
    b_two(1)
    c_three(0)
    a_two(2)
    b_two(2)
    a_three(0)
    b_three(0)
    b_three(1)
    c_four(0)
    c_four(1)
    a_three(1)
    a_three(2)
    b_three(2)
    prep_start()
    prep(0)
    prep(1)
    prep(2)
    prep(3)
    prep(4)
    prep(5)
    prep(6)
    prep(7)
    flat_sq[...] = flat[0]
    c_end_step(0)
    b_end_step(1)
    c_end_step(1)
    b_end_step(0)
    a_end_step(0)
    a_end_step(1)
    a_end_step(2)
    b_end_step(2)

    total = functools.reduce(lambda p, q: p + q, squares)
    n_all[pl.ds(0, 1), :] = jnp.sum(total, axis=0, keepdims=True)
    own = n_all.at[pl.ds(0, 1)]
    rest = n_all.at[pl.ds(1, SHARDS - 1)]
    plane = [[base_x[dx] + base_z[dz] for dz in range(NZ)] for dx in range(NX)]
    inner = [[base_y[dy] + at_c[dc] for dc in range(NC)] for dy in range(NY)]
    for slot, (dx, dz, dy, dc) in enumerate(ALL, 1):
        device = plane[dx][dz] + inner[dy][dc]
        net.start(("norm",), rest, own, n_all.at[pl.ds(slot, 1)], device)
    net.wait(("norm",), rest)
    norm_ref[...] = jnp.sum(n_all[...], axis=0, keepdims=True)
    net.drain()
    assert len(net.slots) == SEMS, len(net.slots)


def reduce_mean(grads, emb, table, row_acc, touched):
    vm = lambda *shape: pltpu.VMEM(shape + (8, LANES), F32)
    shapes = ((8, 1024), (1, LANES), table.shape) + (emb.shape,) * 4 + ((32, LANES),)
    return pl.pallas_call(
        reduce_kernel,
        name="reduce_mean",
        out_shape=[jax.ShapeDtypeStruct(shape, F32) for shape in shapes],
        in_specs=[pl.BlockSpec(memory_space=pltpu.HBM)] * 5,
        out_specs=[pl.BlockSpec(memory_space=pltpu.VMEM)] * len(shapes),
        scratch_shapes=[
            vm(UNITS, NX, NZ, NY),
            vm(UNITS, NX, NZ, NY),
            pltpu.SMEM(touched.shape, jnp.int32),
            pltpu.SMEM(row_acc.shape, F32),
            vm(XS, 2, 4, NY), vm(XS, 2, NZ, NY), vm(XS, 3, NZ), vm(XS, 7),
            vm(YS, 2, NX, 4), vm(YS, 2, NX, NZ), vm(YS, 3, NZ), vm(YS, 7),
            vm(ZS, 2, 2, NY), vm(ZS, 2, 3, NX, NY), vm(ZS, NX * NY - 1),
            pltpu.VMEM((SHARDS, LANES), F32),
            pltpu.SemaphoreType.DMA((SEMS,)),
            pltpu.SemaphoreType.DMA((UNITS + 4,)),
        ],
        compiler_params=pltpu.CompilerParams(
            collective_id=0, has_side_effects=True, vmem_limit_bytes=32 * 1024 * 1024
        ),
    )(*(
        pltpu.with_memory_space_constraint(value, pltpu.HBM)
        for value in (grads.reshape(NX, NZ, NY, NC, 8, 1024), emb, table, row_acc, touched)
    ))


def update_kernel(
    norm_ref, mean_ref, tab_ref, emb_ref, row_tab, row_sq, row_ra, flat_sq,
    param_ref, acc_ref, ra_ref, touched_ref,
    dense_out, dense_acc_out, table_out, row_acc_out, tab,
    idx, rows, dense_new, dense_acc_new, ra_new, sems,
):
    load = pltpu.make_async_copy(touched_ref, idx, sems.at[0])
    load.start()
    norm_sq = jnp.sum(norm_ref[...], axis=1, keepdims=True)
    clip = jnp.minimum(F32(1.0), F32(max_norm) / (jnp.sqrt(norm_sq) + F32(1e-06)))
    square = clip * clip
    live = clip > 0.0

    def grown(old, mean_square):
        return old + jnp.where(live, square * mean_square, 0.0)

    new_ra = grown(row_ra[...], row_sq[...])
    step = (F32(learn_rate) * clip) * emb_ref[...] / (jnp.sqrt(new_ra) + F32(epsilon))
    rows[...] = row_tab[...] - step
    load.wait()

    def sixteen(i, carry):
        for j in range(16):
            t = i * 16 + j
            tab[pl.ds(idx[t], 1), :] = rows[pl.ds(t, 1), :]
        return carry

    lax.fori_loop(0, 32, sixteen, 0)
    out = [pltpu.make_async_copy(tab, table_out, sems.at[1])]
    out[0].start()
    ra_new[...] = grown(ra_ref[...], flat_sq[...])
    scaled = clip * mean_ref[...]
    grow = acc_ref[...] + scaled * scaled
    dense_acc_new[...] = grow
    dense_new[...] = param_ref[...] - F32(learn_rate) * scaled / (jnp.sqrt(grow) + F32(epsilon))
    for i, (src, dst) in enumerate(
        ((ra_new, row_acc_out), (dense_acc_new, dense_acc_out), (dense_new, dense_out))
    ):
        out.append(pltpu.make_async_copy(src, dst, sems.at[2 + i]))
        out[-1].start()
    for copy in out:
        copy.wait()


def body(dense_grads, dense_param, dense_acc, table, row_acc, touched, emb_grads):
    mean, norm, tab, emb, row_tab, row_sq, row_ra, flat_sq = reduce_mean(
        dense_grads, emb_grads, table, row_acc, touched
    )
    vmem, hbm = pl.BlockSpec(memory_space=pltpu.VMEM), pl.BlockSpec(memory_space=pltpu.HBM)
    shapes = (dense_param.shape, dense_param.shape, table.shape, (32, LANES), table.shape)
    new_dense, new_dense_acc, new_table, new_row_acc, _ = pl.pallas_call(
        update_kernel,
        name="update",
        out_shape=[jax.ShapeDtypeStruct(shape, F32) for shape in shapes],
        in_specs=[vmem] * 11 + [hbm],
        out_specs=[hbm] * 4 + [vmem],
        scratch_shapes=[
            pltpu.SMEM(touched.shape, jnp.int32),
            pltpu.VMEM(emb.shape, F32),
            pltpu.VMEM(dense_param.shape, F32),
            pltpu.VMEM(dense_param.shape, F32),
            pltpu.VMEM((32, LANES), F32),
            pltpu.SemaphoreType.DMA((5,)),
        ],
        input_output_aliases={2: 4},
        compiler_params=pltpu.CompilerParams(vmem_limit_bytes=16 * 1024 * 1024),
    )(
        norm, mean, tab, emb, row_tab, row_sq, row_ra, flat_sq,
        dense_param, dense_acc, row_acc.reshape(32, LANES), touched,
    )
    return (new_dense, new_dense_acc, new_table, new_row_acc.reshape(-1))


def solution(mesh):
    return jax.shard_map(
        body,
        mesh=mesh,
        in_specs=(
            P(("gx", "gy"), None, None),
            P(("gx", "gy"), None),
            P(("gx", "gy"), None),
            P(("gx", "gy"), None),
            P(("gx", "gy")),
            P(("gx", "gy")),
            P(("gx", "gy"), None),
        ),
        out_specs=(
            P(("gx", "gy"), None),
            P(("gx", "gy"), None),
            P(("gx", "gy"), None),
            P(("gx", "gy")),
        ),
        check_vma=False,
    )
```

```python
import functools

import jax
import jax.numpy as jnp
from jax import lax
from jax.experimental import pallas as pl
from jax.experimental.pallas import tpu as pltpu
from jax.sharding import PartitionSpec as P

learn_rate = 0.5
max_norm = 8.0
epsilon = 1e-10

LOGICAL = pl.DeviceIdType.LOGICAL
NX, NZ, NY, NC = 4, 8, 4, 2
SHARDS = 256
LANES = 128
F32 = jnp.float32

COLUMN = {"a0": 0, "a1": 1, "a2": 2, "b0": 3, "b1": 4, "b2": 5, "c0": 6, "c1": 7, "c2": (2, 5)}
WHOLE, MOST, REST = (8, LANES), (3, 2, LANES), (2, 2, LANES)
TILE = {u: WHOLE for u in COLUMN} | {"a2": MOST, "b2": MOST, "c2": REST}
WAVES = 3
SEMS, SENT_ROWS = 71, 16575

ORDER = (
    "b_far0", "a_far0", "c_zero0", "c_zero2", "b_far1", "b_far2", "a_near0", "a_far1", "c_zero1", "c_near0",
    "c_near2", "b_near1", "c_one0", "c_one2", "c_near1", "b_near0", "a_late0", "b_late0", "a_far2", "a_near1",
    "b_late1", "c_one1", "a_late1", "c_two0", "b_near2", "a_near2", "c_two2", "b_late2", "c_two1", "a_late2",
    "c_three0", "a_two0", "b_two1", "a_two1", "c_three2", "b_two0", "c_three1", "b_two2", "a_two2", "c_four0",
    "a_three0", "b_three1", "a_three1", "c_four2", "b_three0", "c_four1", "a_three2", "b_three2", "prep0",
    "prep1", "prep2", "prep3", "prep4", "prep5", "prep6", "prep7", "c_end0", "b_end0", "c_end2", "a_end0",
    "a_end1", "b_end1", "c_end1", "a_end2", "b_end2",
)

PLANE = sorted(
    [(dx, dy) for dx in range(NX) for dy in range(NY) if dx or dy],
    key=lambda d: -(min(d[0], NX - d[0]) + min(d[1], NY - d[1])),
)


def hops(dx, dy, dz):
    return min(dx, NX - dx) + min(dy, NY - dy) + min(dz, NZ - dz)


ALL = sorted(
    [
        (dx, dz, dy, dc)
        for dx in range(NX) for dz in range(NZ) for dy in range(NY) for dc in range(NC)
        if dx or dz or dy or dc
    ],
    key=lambda d: -hops(d[0], d[2], d[1]),
)


def size(ref):
    rows = 1
    for n in ref.shape[:-1]:
        rows *= n
    return rows


class Net:
    def __init__(self, sems, tally, mate):
        self.sems, self.tally, self.mate = sems, tally, mate
        self.slots, self.rows = {"sent": 0}, 0

    def sem(self, name):
        return self.sems.at[self.slots.setdefault(name, len(self.slots))]

    def start(self, name, src, dst, device):
        self.rows += size(src)
        pltpu.make_async_remote_copy(
            src_ref=src,
            dst_ref=dst,
            send_sem=self.sem("sent"),
            recv_sem=self.sem(name),
            device_id=device,
            device_id_type=LOGICAL,
        ).start()

    def filled(self, ref, name):
        return pltpu.make_async_remote_copy(
            src_ref=ref,
            dst_ref=ref,
            send_sem=self.sem("sent"),
            recv_sem=self.sem(name),
            device_id=self.mate,
            device_id_type=LOGICAL,
        )

    def wait(self, name, ref):
        self.filled(ref, name).wait_recv()

    def drain(self):
        self.filled(self.tally.at[pl.ds(0, self.rows)], "sent").wait_send()


def buffers(u):
    vm = lambda *shape: pltpu.VMEM(shape + TILE[u], F32)
    out = {"sum": vm(NX, NZ, NY), "pair": vm(NX, NZ, NY)}
    if u[0] == "a":
        out |= {"relay": vm(2, 4, NY), "last": vm(2, NZ, NY), "mid": vm(3, NZ), "end": vm(NZ - 1)}
    elif u[0] == "b":
        out |= {"relay": vm(2, NX, 4), "last": vm(2, NX, NZ), "mid": vm(3, NZ), "end": vm(NZ - 1)}
    else:
        out |= {"far": vm(2, 2, NY), "chain": vm(3, 2, NX, NY), "end": vm(NX * NY - 1)}
    return out


def reduce_kernel(
    g_ref, half_ref, e_ref, table_ref, row_acc_ref, touched_ref,
    mean_ref, norm_ref, tab, emb, row_tab, row_sq, row_ra, flat_sq,
    units, idx, ra, n_all, tally, net_sems, load_sems,
):
    gx, gy = lax.axis_index("gx"), lax.axis_index("gy")
    x, z = lax.div(gx, NZ), lax.rem(gx, NZ)
    y, c = lax.div(gy, NC), lax.rem(gy, NC)
    at_x = [x] + [lax.rem(x + d, NX) for d in range(1, NX)]
    at_y = [y] + [lax.rem(y + d, NY) for d in range(1, NY)]
    at_z = [z] + [lax.rem(z + d, NZ) for d in range(1, NZ)]
    at_c = [c, 1 - c]
    base_x = [v * (NZ * NY * NC) for v in at_x]
    base_z = [v * (NY * NC) for v in at_z]
    base_y = [v * NC for v in at_y]

    def dev(dx=0, dy=0, dz=0, dc=0):
        return base_x[dx % NX] + base_z[dz % NZ] + (base_y[dy % NY] + at_c[dc])

    every = slice(None)

    def rows_of(u, buffer, spot, core):
        if TILE[u] == WHOLE:
            return [(g_ref.at[(*spot, core, COLUMN[u])], buffer.at[spot])]
        if TILE[u] == MOST:
            return [(half_ref.at[(*spot, core, COLUMN[u], pl.ds(0, 3))], buffer.at[spot])]
        return [
            (half_ref.at[(*spot, core, column, 3)], buffer.at[(*spot, i)])
            for i, column in enumerate(COLUMN[u])
        ]

    loads, count = {}, 0
    for name in ORDER:
        u = name[0] + name[-1]
        if u in COLUMN and u not in loads:
            loads[u] = []
            for src, dst in rows_of(u, units[u]["sum"], (every, every, every), c):
                loads[u].append(pltpu.make_async_copy(src, dst, load_sems.at[count]))
                loads[u][-1].start()
                count += 1
    prep_loads = [
        pltpu.make_async_copy(src, dst, load_sems.at[count + i])
        for i, (src, dst) in enumerate(
            ((e_ref, emb), (touched_ref, idx), (row_acc_ref, ra), (table_ref, tab))
        )
    ]
    for copy in prep_loads:
        copy.start()

    barrier = pltpu.get_barrier_semaphore()
    nearby = [dev(dc=1)] + [dev(**{axis: step}) for axis in ("dx", "dy", "dz") for step in (1, -1)]
    for device in nearby:
        pl.semaphore_signal(barrier, inc=1, device_id=device, device_id_type=LOGICAL)
    pl.semaphore_wait(barrier, len(nearby))

    mate = dev(dc=1)
    net = Net(net_sems, tally, mate)

    def spot(u, k):
        if u[0] == "a":
            return (at_x[k], every, every)
        if u[0] == "b":
            return (every, every, at_y[k])
        return (every, at_z[k], every)

    FAR, NEAR, OWN = (2,), (1, 3), (0,)
    NEEDS = {
        "a_far": FAR, "a_near": NEAR, "a_two": OWN, "b_far": FAR, "b_near": NEAR, "b_two": OWN,
        "c_zero": (4,), "c_near": (3, 5), "c_two": (2, 6), "c_three": (1, 7, 0),
    }
    for name in ORDER:
        u = name[0] + name[-1]
        for k in NEEDS.get(name[:-1], ()):
            for src, dst in rows_of(u, units[u]["pair"], spot(u, k), at_c[1]):
                net.start(("pair", name), src, dst, mate)

    def take(name):
        u, ks = name[0] + name[-1], NEEDS.get(name[:-1], ())
        if not ks:
            return
        for copy in loads.pop(u, ()):
            copy.wait()
        some = pl.ds(0, len(ks))
        span = {"a": (some,), "b": (every, every, some), "c": (every, some)}[u[0]]
        net.wait(("pair", name), units[u]["pair"].at[span])
        for k in ks:
            mine = units[u]["sum"].at[spot(u, k)]
            mine[...] = mine[...] + units[u]["pair"].at[spot(u, k)][...]

    LO, HI = pl.ds(0, 4), pl.ds(4, 4)

    def view(u, k, half):
        total = units[u]["sum"]
        return total.at[at_x[k], half] if u[0] == "a" else total.at[:, half, at_y[k]]

    def land(u, side, half):
        last = units[u]["last"]
        return last.at[side, half] if u[0] == "a" else last.at[side, :, half]

    def first_axis(u, step):
        return dev(dx=step) if u[0] == "a" else dev(dy=step)

    def far(u):
        for side, half in enumerate((LO, HI)):
            net.start(("relay", u), view(u, 2, half), units[u]["relay"].at[side], first_axis(u, 1 - 2 * side))

    def near(u):
        for side, k, half in ((0, 1, HI), (1, 3, LO)):
            net.start(("last", u), view(u, k, half), land(u, side, half), first_axis(u, 1 - 2 * side))

    def late(u):
        relay = units[u]["relay"]
        net.wait(("relay", u), relay)
        for side, k, half in ((0, 1, LO), (1, 3, HI)):
            ref = view(u, k, half)
            ref[...] = ref[...] + relay[side]
            net.start(("last", u), ref, land(u, side, half), first_axis(u, 1 - 2 * side))

    def two(u):
        last, total = units[u]["last"], units[u]["sum"]
        net.wait(("last", u), last)
        ref = total.at[spot(u, 0)]
        ref[...] = ref[...] + (last[0] + last[1])
        for k in (2, 1, 3):
            if u[0] == "a":
                src, device = total.at[x, :, at_y[k]], dev(dy=k)
            else:
                src, device = total.at[at_x[k], :, y], dev(dx=k)
            net.start(("mid", u), src, units[u]["mid"].at[k - 1], device)

    def three(u):
        mid, total = units[u]["mid"], units[u]["sum"]
        net.wait(("mid", u), mid)
        ref = total.at[x, :, y]
        ref[...] = ref[...] + (mid[0] + mid[1] + mid[2])
        for k in (4, 3, 5, 2, 6, 1, 7):
            net.start(("end", u), total.at[x, at_z[k], y], units[u]["end"].at[k - 1], dev(dz=k))

    XLO, XHI = pl.ds(0, 2), pl.ds(2, 2)

    def c_part(u, k, half=every):
        return units[u]["sum"].at[half, at_z[k]]

    def c_zero(u):
        for side, half in enumerate((XLO, XHI)):
            net.start(("far", u), c_part(u, 4, half), units[u]["far"].at[side], dev(dz=1 - 2 * side))

    def c_near(u):
        for side, k, half in ((0, 3, XHI), (1, 5, XLO)):
            net.start(("chain", u, 0), c_part(u, k, half), units[u]["chain"].at[0, side, half], dev(dz=1 - 2 * side))

    def c_one(u):
        net.wait(("far", u), units[u]["far"])
        for side, k, half in ((0, 3, XLO), (1, 5, XHI)):
            ref = c_part(u, k, half)
            ref[...] = ref[...] + units[u]["far"][side]
            net.start(("chain", u, 0), ref, units[u]["chain"].at[0, side, half], dev(dz=1 - 2 * side))

    def c_pass(u, step, ks):
        chain = units[u]["chain"]
        net.wait(("chain", u, step), chain.at[step])
        for side, k in enumerate(ks):
            ref = c_part(u, k)
            ref[...] = ref[...] + chain[step, side]
            net.start(("chain", u, step + 1), ref, chain.at[step + 1, side], dev(dz=1 - 2 * side))

    def c_four(u):
        chain = units[u]["chain"]
        net.wait(("chain", u, 2), chain.at[2])
        ref = c_part(u, 0)
        ref[...] = ref[...] + (chain[2, 0] + chain[2, 1])
        for dx, dy in PLANE:
            net.start(
                ("end", u), units[u]["sum"].at[at_x[dx], z, at_y[dy]],
                units[u]["end"].at[dx * NY + dy - 1], dev(dx=dx, dy=dy),
            )

    squares = []

    def end(u):
        ends = units[u]["end"]
        net.wait(("end", u), ends)
        mean = (units[u]["sum"][x, z, y] + jnp.sum(ends[...], axis=0)) / F32(SHARDS)
        cols = lambda column: pl.ds(column * LANES, LANES)
        if TILE[u] == WHOLE:
            mean_ref[:, cols(COLUMN[u])] = mean
            squares.append(jnp.sum(mean * mean, axis=0, keepdims=True))
            return
        for i in range(TILE[u][0]):
            row, column = (2 * i, COLUMN[u]) if TILE[u] == MOST else (6, COLUMN[u][i])
            mean_ref[pl.ds(row, 2), cols(column)] = mean[i]
            squares.append(jnp.sum(mean[i] * mean[i], axis=0, keepdims=True))

    def prep_start():
        for copy in prep_loads:
            copy.wait()
        grads = emb[...]
        own = grads * grads
        squares.append(jnp.sum(own, axis=0, keepdims=True))
        mean = jnp.sum(own, axis=1, keepdims=True) / F32(LANES)
        row_sq[...] = jnp.broadcast_to(mean, row_sq.shape)

    place = lax.broadcasted_iota(jnp.int32, (32, LANES), 0) * LANES
    place = place + lax.broadcasted_iota(jnp.int32, (32, LANES), 1)
    flat = [jnp.zeros((32, LANES), F32)]

    def prep(part, parts=8):
        size = 512 // parts
        if part == 0:
            prep_start()

        def eight(i, total):
            base = part * size + i * 8
            for j in range(8):
                t = base + j
                r = idx[t]
                row_tab[pl.ds(t, 1), :] = tab[pl.ds(r, 1), :]
                row_ra[pl.ds(t, 1), :] = jnp.full((1, LANES), ra[r], F32)
                total = jnp.where(place == r, row_sq[pl.ds(t, 1), :], total)
            return total

        flat[0] = lax.fori_loop(0, size // 8, eight, flat[0])
        if part == parts - 1:
            flat_sq[...] = flat[0]

    steps = {
        "a_far": far, "a_near": near, "a_late": late, "a_two": two, "a_three": three, "a_end": end,
        "b_far": far, "b_near": near, "b_late": late, "b_two": two, "b_three": three, "b_end": end,
        "c_zero": c_zero, "c_near": c_near, "c_one": c_one,
        "c_two": lambda u: c_pass(u, 0, (2, 6)), "c_three": lambda u: c_pass(u, 1, (1, 7)),
        "c_four": c_four, "c_end": end,
    }
    for name in ORDER:
        with jax.named_scope(name):
            if name[:4] == "prep":
                prep(int(name[4:]))
            else:
                take(name)
                steps[name[:-1]](name[0] + name[-1])

    n_all[pl.ds(0, 1), :] = functools.reduce(lambda p, q: p + q, squares)
    own = n_all.at[pl.ds(0, 1)]
    rest = n_all.at[pl.ds(1, SHARDS - 1)]
    plane = [[base_x[dx] + base_z[dz] for dz in range(NZ)] for dx in range(NX)]
    inner = [[base_y[dy] + at_c[dc] for dc in range(NC)] for dy in range(NY)]
    for slot, (dx, dz, dy, dc) in enumerate(ALL, 1):
        device = plane[dx][dz] + inner[dy][dc]
        net.start("norm", own, n_all.at[pl.ds(slot, 1)], device)
    with jax.named_scope("nwait"):
        net.wait("norm", rest)
    norm_ref[...] = jnp.sum(n_all[...], axis=0, keepdims=True)
    with jax.named_scope("drain"):
        net.drain()
    assert (len(net.slots), net.rows) == (SEMS, SENT_ROWS), (len(net.slots), net.rows)


def reduce_mean(grads, emb, table, row_acc, touched):
    shapes = ((8, 1024), (1, LANES), table.shape) + (emb.shape,) * 4 + ((32, LANES),)
    tiles = grads.reshape(SHARDS, 8, 8, LANES).transpose(0, 2, 1, 3)
    return pl.pallas_call(
        reduce_kernel,
        name="reduce_mean",
        out_shape=[jax.ShapeDtypeStruct(shape, F32) for shape in shapes],
        in_specs=[pl.BlockSpec(memory_space=pltpu.HBM)] * 6,
        out_specs=[pl.BlockSpec(memory_space=pltpu.VMEM)] * len(shapes),
        scratch_shapes=[
            {u: buffers(u) for u in COLUMN},
            pltpu.SMEM(touched.shape, jnp.int32),
            pltpu.SMEM(row_acc.shape, F32),
            pltpu.VMEM((SHARDS, LANES), F32),
            pltpu.VMEM((SENT_ROWS, LANES), F32),
            pltpu.SemaphoreType.DMA((SEMS,)),
            pltpu.SemaphoreType.DMA((len(COLUMN) + 1 + 4,)),
        ],
        compiler_params=pltpu.CompilerParams(
            collective_id=0, has_side_effects=True, vmem_limit_bytes=40 * 1024 * 1024
        ),
    )(*(
        pltpu.with_memory_space_constraint(value, pltpu.HBM)
        for value in (
            tiles.reshape(NX, NZ, NY, NC, 8, *WHOLE),
            tiles.reshape(NX, NZ, NY, NC, 8, 4, 2, LANES),
            emb, table, row_acc, touched,
        )
    ))


def update_kernel(
    norm_ref, mean_ref, tab_ref, emb_ref, row_tab, row_sq, row_ra, flat_sq,
    param_ref, acc_ref, ra_ref, touched_ref,
    dense_out, dense_acc_out, table_out, row_acc_out, tab,
    idx, rows, dense_new, dense_acc_new, ra_new, sems,
):
    load = pltpu.make_async_copy(touched_ref, idx, sems.at[0])
    load.start()
    norm_sq = jnp.sum(norm_ref[...], axis=1, keepdims=True)
    clip = jnp.minimum(F32(1.0), F32(max_norm) / (jnp.sqrt(norm_sq) + F32(1e-06)))
    square = clip * clip
    live = clip > 0.0

    def grown(old, mean_square):
        return old + jnp.where(live, square * mean_square, 0.0)

    new_ra = grown(row_ra[...], row_sq[...])
    step = (F32(learn_rate) * clip) * emb_ref[...] / (jnp.sqrt(new_ra) + F32(epsilon))
    rows[...] = row_tab[...] - step
    load.wait()

    def sixteen(i, carry):
        for j in range(16):
            t = i * 16 + j
            tab[pl.ds(idx[t], 1), :] = rows[pl.ds(t, 1), :]
        return carry

    lax.fori_loop(0, 32, sixteen, 0)
    out = [pltpu.make_async_copy(tab, table_out, sems.at[1])]
    out[0].start()
    ra_new[...] = grown(ra_ref[...], flat_sq[...])
    scaled = clip * mean_ref[...]
    grow = acc_ref[...] + scaled * scaled
    dense_acc_new[...] = grow
    dense_new[...] = param_ref[...] - F32(learn_rate) * scaled / (jnp.sqrt(grow) + F32(epsilon))
    for i, (src, dst) in enumerate(
        ((ra_new, row_acc_out), (dense_acc_new, dense_acc_out), (dense_new, dense_out))
    ):
        out.append(pltpu.make_async_copy(src, dst, sems.at[2 + i]))
        out[-1].start()
    for copy in out:
        copy.wait()


def body(dense_grads, dense_param, dense_acc, table, row_acc, touched, emb_grads):
    mean, norm, tab, emb, row_tab, row_sq, row_ra, flat_sq = reduce_mean(
        dense_grads, emb_grads, table, row_acc, touched
    )
    vmem, hbm = pl.BlockSpec(memory_space=pltpu.VMEM), pl.BlockSpec(memory_space=pltpu.HBM)
    shapes = (dense_param.shape, dense_param.shape, table.shape, (32, LANES), table.shape)
    new_dense, new_dense_acc, new_table, new_row_acc, _ = pl.pallas_call(
        update_kernel,
        name="update",
        out_shape=[jax.ShapeDtypeStruct(shape, F32) for shape in shapes],
        in_specs=[vmem] * 11 + [hbm],
        out_specs=[hbm] * 4 + [vmem],
        scratch_shapes=[
            pltpu.SMEM(touched.shape, jnp.int32),
            pltpu.VMEM(emb.shape, F32),
            pltpu.VMEM(dense_param.shape, F32),
            pltpu.VMEM(dense_param.shape, F32),
            pltpu.VMEM((32, LANES), F32),
            pltpu.SemaphoreType.DMA((5,)),
        ],
        input_output_aliases={2: 4},
        compiler_params=pltpu.CompilerParams(vmem_limit_bytes=16 * 1024 * 1024),
    )(
        norm, mean, tab, emb, row_tab, row_sq, row_ra, flat_sq,
        dense_param, dense_acc, row_acc.reshape(32, LANES), touched,
    )
    return (new_dense, new_dense_acc, new_table, new_row_acc.reshape(-1))


def solution(mesh):
    return jax.shard_map(
        body,
        mesh=mesh,
        in_specs=(
            P(("gx", "gy"), None, None),
            P(("gx", "gy"), None),
            P(("gx", "gy"), None),
            P(("gx", "gy"), None),
            P(("gx", "gy")),
            P(("gx", "gy")),
            P(("gx", "gy"), None),
        ),
        out_specs=(
            P(("gx", "gy"), None),
            P(("gx", "gy"), None),
            P(("gx", "gy"), None),
            P(("gx", "gy")),
        ),
        check_vma=False,
    )
```

```python
import functools

import jax
import jax.numpy as jnp
from jax import lax
from jax.experimental import pallas as pl
from jax.experimental.pallas import tpu as pltpu
from jax.sharding import PartitionSpec as P

learn_rate = 0.5
max_norm = 8.0
epsilon = 1e-10

LOGICAL = pl.DeviceIdType.LOGICAL
NX, NZ, NY, NC = 4, 8, 4, 2
SHARDS = 256
LANES = 128
F32 = jnp.float32

UNITS = {
    "a0": (0, None), "a1": (1, None), "a2": (2, 0),
    "b0": (3, None), "b1": (4, None), "b2": (5, 0),
    "c0": (2, 1), "c1": (5, 1), "c2": (6, None), "c3": (7, None),
}
TILE = {u: (8, LANES) if rows is None else (4, LANES) for u, (_, rows) in UNITS.items()}
SEMS, SENT_ROWS = 70, 16575

ORDER = (
    "c_zero1", "a_far2", "c_zero2", "b_far2", "c_near1", "b_far1", "c_zero0", "c_near0", "c_zero3", "a_near2",
    "c_near2", "a_far0", "b_near2", "b_far0", "b_near0", "a_near0", "c_one1", "c_one2", "a_late2", "b_late2",
    "c_one0", "c_near3", "b_near1", "a_far1", "c_one3", "b_late1", "a_late0", "c_two1", "c_two2", "c_two0",
    "a_near1", "b_late0", "c_two3", "a_late1", "c_three1", "a_two2", "b_two2", "b_two1", "a_two0", "c_three2",
    "c_three0", "b_two0", "c_three3", "a_two1", "a_three2", "b_three1", "b_three2", "c_four2", "a_three0",
    "c_four0", "b_three0", "c_four1", "c_four3", "a_three1",
    "c_end2", "c_end1", "b_end1", "a_end0", "b_end0", "a_end2", "b_end2", "c_end0",
    "a_end1", "c_end3",
)

PLANE = sorted(
    [(dx, dy) for dx in range(NX) for dy in range(NY) if dx or dy],
    key=lambda d: -(min(d[0], NX - d[0]) + min(d[1], NY - d[1])),
)


def hops(dx, dy, dz):
    return min(dx, NX - dx) + min(dy, NY - dy) + min(dz, NZ - dz)


ALL = sorted(
    [
        (dx, dz, dy, dc)
        for dx in range(NX) for dz in range(NZ) for dy in range(NY) for dc in range(NC)
        if dx or dz or dy or dc
    ],
    key=lambda d: -hops(d[0], d[2], d[1]),
)


def size(ref):
    rows = 1
    for n in ref.shape[:-1]:
        rows *= n
    return rows


class Net:
    def __init__(self, sems, tally, mate):
        self.sems, self.tally, self.mate = sems, tally, mate
        self.slots, self.rows = {"sent": 0}, 0

    def sem(self, name):
        return self.sems.at[self.slots.setdefault(name, len(self.slots))]

    def start(self, name, src, dst, device):
        self.rows += size(src)
        pltpu.make_async_remote_copy(
            src_ref=src,
            dst_ref=dst,
            send_sem=self.sem("sent"),
            recv_sem=self.sem(name),
            device_id=device,
            device_id_type=LOGICAL,
        ).start()

    def filled(self, ref, name):
        return pltpu.make_async_remote_copy(
            src_ref=ref,
            dst_ref=ref,
            send_sem=self.sem("sent"),
            recv_sem=self.sem(name),
            device_id=self.mate,
            device_id_type=LOGICAL,
        )

    def wait(self, name, ref):
        self.filled(ref, name).wait_recv()

    def drain(self):
        self.filled(self.tally.at[pl.ds(0, self.rows)], "sent").wait_send()


def buffers(u):
    vm = lambda *shape: pltpu.VMEM(shape + TILE[u], F32)
    out = {"sum": vm(NX, NZ, NY), "pair": vm(NX, NZ, NY)}
    if u[0] == "a":
        out |= {"relay": vm(2, 4, NY), "last": vm(2, NZ, NY), "mid": vm(3, NZ), "end": vm(NZ - 1)}
    elif u[0] == "b":
        out |= {"relay": vm(2, NX, 4), "last": vm(2, NX, NZ), "mid": vm(3, NZ), "end": vm(NZ - 1)}
    else:
        out |= {"far": vm(2, 2, NY), "chain": vm(3, 2, NX, NY), "end": vm(NX * NY - 1)}
    return out


def reduce_kernel(
    g_ref, half_ref, e_ref, table_ref, row_acc_ref, touched_ref,
    mean_ref, norm_ref, tab, emb, row_tab, row_sq, row_ra, flat_sq,
    units, idx, ra, n_all, tally, net_sems, load_sems,
):
    gx, gy = lax.axis_index("gx"), lax.axis_index("gy")
    x, z = lax.div(gx, NZ), lax.rem(gx, NZ)
    y, c = lax.div(gy, NC), lax.rem(gy, NC)
    at_x = [x] + [lax.rem(x + d, NX) for d in range(1, NX)]
    at_y = [y] + [lax.rem(y + d, NY) for d in range(1, NY)]
    at_z = [z] + [lax.rem(z + d, NZ) for d in range(1, NZ)]
    at_c = [c, 1 - c]
    base_x = [v * (NZ * NY * NC) for v in at_x]
    base_z = [v * (NY * NC) for v in at_z]
    base_y = [v * NC for v in at_y]

    def dev(dx=0, dy=0, dz=0, dc=0):
        return base_x[dx % NX] + base_z[dz % NZ] + (base_y[dy % NY] + at_c[dc])

    every = slice(None)

    barrier = pltpu.get_barrier_semaphore()
    nearby = [dev(dc=1)] + [dev(**{axis: step}) for axis in ("dx", "dy", "dz") for step in (1, -1)]
    for device in nearby:
        pl.semaphore_signal(barrier, inc=1, device_id=device, device_id_type=LOGICAL)

    def rows_of(u, spot, core):
        column, rows = UNITS[u]
        if rows is None:
            return g_ref.at[(*spot, core, column)]
        return half_ref.at[(*spot, core, column, rows)]

    loads = {}
    for name in ORDER:
        u = name[0] + name[-1]
        if u in UNITS and u not in loads:
            loads[u] = pltpu.make_async_copy(
                rows_of(u, (every, every, every), c), units[u]["sum"], load_sems.at[len(loads)]
            )
            loads[u].start()
    prep_loads = [
        pltpu.make_async_copy(src, dst, load_sems.at[len(UNITS) + i])
        for i, (src, dst) in enumerate(
            ((e_ref, emb), (touched_ref, idx), (row_acc_ref, ra), (table_ref, tab))
        )
    ]
    for copy in prep_loads:
        copy.start()

    pl.semaphore_wait(barrier, len(nearby))

    mate = dev(dc=1)
    net = Net(net_sems, tally, mate)

    def spot(u, k):
        if u[0] == "a":
            return (at_x[k], every, every)
        if u[0] == "b":
            return (every, every, at_y[k])
        return (every, at_z[k], every)

    FAR, NEAR = (2,), (1, 3, 0)
    NEEDS = {
        "a_far": FAR, "a_near": NEAR, "b_far": FAR, "b_near": NEAR,
        "c_zero": (4,), "c_near": (3, 5), "c_two": (2, 6, 1, 7, 0),
    }
    for name in ORDER:
        u = name[0] + name[-1]
        for k in NEEDS.get(name[:-1], ()):
            src = rows_of(u, spot(u, k), at_c[1])
            net.start(("pair", name), src, units[u]["pair"].at[spot(u, k)], mate)

    def take(name):
        u, ks = name[0] + name[-1], NEEDS.get(name[:-1], ())
        if not ks:
            return
        if u in loads:
            loads.pop(u).wait()
        some = pl.ds(0, len(ks))
        span = {"a": (some,), "b": (every, every, some), "c": (every, some)}[u[0]]
        net.wait(("pair", name), units[u]["pair"].at[span])
        for k in ks:
            mine = units[u]["sum"].at[spot(u, k)]
            mine[...] = mine[...] + units[u]["pair"].at[spot(u, k)][...]

    LO, HI = pl.ds(0, 4), pl.ds(4, 4)

    def view(u, k, half):
        total = units[u]["sum"]
        return total.at[at_x[k], half] if u[0] == "a" else total.at[:, half, at_y[k]]

    def land(u, side, half):
        last = units[u]["last"]
        return last.at[side, half] if u[0] == "a" else last.at[side, :, half]

    def first_axis(u, step):
        return dev(dx=step) if u[0] == "a" else dev(dy=step)

    def far(u):
        for side, half in enumerate((LO, HI)):
            net.start(("relay", u), view(u, 2, half), units[u]["relay"].at[side], first_axis(u, 1 - 2 * side))

    def near(u):
        for side, k, half in ((0, 1, HI), (1, 3, LO)):
            net.start(("last", u), view(u, k, half), land(u, side, half), first_axis(u, 1 - 2 * side))

    def late(u):
        relay = units[u]["relay"]
        net.wait(("relay", u), relay)
        for side, k, half in ((0, 1, LO), (1, 3, HI)):
            ref = view(u, k, half)
            ref[...] = ref[...] + relay[side]
            net.start(("last", u), ref, land(u, side, half), first_axis(u, 1 - 2 * side))

    def two(u):
        last, total = units[u]["last"], units[u]["sum"]
        net.wait(("last", u), last)
        ref = total.at[spot(u, 0)]
        ref[...] = ref[...] + (last[0] + last[1])
        for k in (2, 1, 3):
            if u[0] == "a":
                src, device = total.at[x, :, at_y[k]], dev(dy=k)
            else:
                src, device = total.at[at_x[k], :, y], dev(dx=k)
            net.start(("mid", u), src, units[u]["mid"].at[k - 1], device)

    def three(u):
        mid, total = units[u]["mid"], units[u]["sum"]
        net.wait(("mid", u), mid)
        ref = total.at[x, :, y]
        ref[...] = ref[...] + (mid[0] + mid[1] + mid[2])
        for k in (4, 3, 5, 2, 6, 1, 7):
            net.start(("end", u), total.at[x, at_z[k], y], units[u]["end"].at[k - 1], dev(dz=k))

    XLO, XHI = pl.ds(0, 2), pl.ds(2, 2)

    def c_part(u, k, half=every):
        return units[u]["sum"].at[half, at_z[k]]

    def c_zero(u):
        for side, half in enumerate((XLO, XHI)):
            net.start(("far", u), c_part(u, 4, half), units[u]["far"].at[side], dev(dz=1 - 2 * side))

    def c_near(u):
        for side, k, half in ((0, 3, XHI), (1, 5, XLO)):
            net.start(("chain", u, 0), c_part(u, k, half), units[u]["chain"].at[0, side, half], dev(dz=1 - 2 * side))

    def c_one(u):
        net.wait(("far", u), units[u]["far"])
        for side, k, half in ((0, 3, XLO), (1, 5, XHI)):
            ref = c_part(u, k, half)
            ref[...] = ref[...] + units[u]["far"][side]
            net.start(("chain", u, 0), ref, units[u]["chain"].at[0, side, half], dev(dz=1 - 2 * side))

    def c_pass(u, step, ks):
        chain = units[u]["chain"]
        net.wait(("chain", u, step), chain.at[step])
        for side, k in enumerate(ks):
            ref = c_part(u, k)
            ref[...] = ref[...] + chain[step, side]
            net.start(("chain", u, step + 1), ref, chain.at[step + 1, side], dev(dz=1 - 2 * side))

    def c_four(u):
        chain = units[u]["chain"]
        net.wait(("chain", u, 2), chain.at[2])
        ref = c_part(u, 0)
        ref[...] = ref[...] + (chain[2, 0] + chain[2, 1])
        for dx, dy in PLANE:
            net.start(
                ("end", u), units[u]["sum"].at[at_x[dx], z, at_y[dy]],
                units[u]["end"].at[dx * NY + dy - 1], dev(dx=dx, dy=dy),
            )

    squares = []

    def end(u):
        ends = units[u]["end"]
        net.wait(("end", u), ends)
        mean = (units[u]["sum"][x, z, y] + jnp.sum(ends[...], axis=0)) / F32(SHARDS)
        column, rows = UNITS[u]
        spot = slice(None) if rows is None else pl.ds(4 * rows, 4)
        mean_ref[spot, pl.ds(column * LANES, LANES)] = mean
        squares.append(jnp.sum(mean * mean, axis=0, keepdims=True))

    def prep_start():
        for copy in prep_loads:
            copy.wait()
        grads = emb[...]
        own = grads * grads
        squares.append(jnp.sum(own, axis=0, keepdims=True))
        mean = jnp.sum(own, axis=1, keepdims=True) / F32(LANES)
        row_sq[...] = jnp.broadcast_to(mean, row_sq.shape)

    place = lax.broadcasted_iota(jnp.int32, (32, LANES), 0) * LANES
    place = place + lax.broadcasted_iota(jnp.int32, (32, LANES), 1)
    flat = [jnp.zeros((32, LANES), F32)]

    def prep(part, parts=8):
        size = 512 // parts
        def eight(i, total):
            base = part * size + i * 8
            for j in range(8):
                t = base + j
                r = idx[t]
                row_tab[pl.ds(t, 1), :] = tab[pl.ds(r, 1), :]
                row_ra[pl.ds(t, 1), :] = jnp.full((1, LANES), ra[r], F32)
                total = jnp.where(place == r, row_sq[pl.ds(t, 1), :], total)
            return total

        flat[0] = lax.fori_loop(0, size // 8, eight, flat[0])
        if part == parts - 1:
            flat_sq[...] = flat[0]

    steps = {
        "a_far": far, "a_near": near, "a_late": late, "a_two": two, "a_three": three, "a_end": end,
        "b_far": far, "b_near": near, "b_late": late, "b_two": two, "b_three": three, "b_end": end,
        "c_zero": c_zero, "c_near": c_near, "c_one": c_one,
        "c_two": lambda u: c_pass(u, 0, (2, 6)), "c_three": lambda u: c_pass(u, 1, (1, 7)),
        "c_four": c_four, "c_end": end,
    }
    for name in ORDER:
        with jax.named_scope(name):
            take(name)
            steps[name[:-1]](name[0] + name[-1])
        if name == ORDER[-len(UNITS) - 1]:
            prep_start()

    n_all[pl.ds(0, 1), :] = functools.reduce(lambda p, q: p + q, squares)
    own = n_all.at[pl.ds(0, 1)]
    rest = n_all.at[pl.ds(1, SHARDS - 1)]
    plane = [[base_x[dx] + base_z[dz] for dz in range(NZ)] for dx in range(NX)]
    inner = [[base_y[dy] + at_c[dc] for dc in range(NC)] for dy in range(NY)]
    for slot, (dx, dz, dy, dc) in enumerate(ALL, 1):
        device = plane[dx][dz] + inner[dy][dc]
        net.start("norm", own, n_all.at[pl.ds(slot, 1)], device)
    for part in range(8):
        prep(part)
    with jax.named_scope("nwait"):
        net.wait("norm", rest)
    norm_ref[...] = jnp.sum(n_all[...], axis=0, keepdims=True)
    with jax.named_scope("drain"):
        net.drain()
    assert (len(net.slots), net.rows) == (SEMS, SENT_ROWS), (len(net.slots), net.rows)


def reduce_mean(grads, emb, table, row_acc, touched):
    shapes = ((8, 1024), (1, LANES), table.shape) + (emb.shape,) * 4 + ((32, LANES),)
    tiles = grads.reshape(SHARDS, 8, 8, LANES).transpose(0, 2, 1, 3)
    return pl.pallas_call(
        reduce_kernel,
        name="reduce_mean",
        out_shape=[jax.ShapeDtypeStruct(shape, F32) for shape in shapes],
        in_specs=[pl.BlockSpec(memory_space=pltpu.HBM)] * 6,
        out_specs=[pl.BlockSpec(memory_space=pltpu.VMEM)] * len(shapes),
        scratch_shapes=[
            {u: buffers(u) for u in UNITS},
            pltpu.SMEM(touched.shape, jnp.int32),
            pltpu.SMEM(row_acc.shape, F32),
            pltpu.VMEM((SHARDS, LANES), F32),
            pltpu.VMEM((SENT_ROWS, LANES), F32),
            pltpu.SemaphoreType.DMA((SEMS,)),
            pltpu.SemaphoreType.DMA((len(UNITS) + 4,)),
        ],
        compiler_params=pltpu.CompilerParams(
            collective_id=0, has_side_effects=True, vmem_limit_bytes=40 * 1024 * 1024
        ),
    )(*(
        pltpu.with_memory_space_constraint(value, pltpu.HBM)
        for value in (
            tiles.reshape(NX, NZ, NY, NC, 8, 8, LANES),
            tiles.reshape(NX, NZ, NY, NC, 8, 2, 4, LANES),
            emb, table, row_acc, touched,
        )
    ))


def update_kernel(
    norm_ref, mean_ref, tab_ref, emb_ref, row_tab, row_sq, row_ra, flat_sq,
    param_ref, acc_ref, ra_ref, touched_ref,
    dense_out, dense_acc_out, table_out, row_acc_out, tab,
    idx, rows, dense_new, dense_acc_new, ra_new, sems,
):
    load = pltpu.make_async_copy(touched_ref, idx, sems.at[0])
    load.start()
    norm_sq = jnp.sum(norm_ref[...], axis=1, keepdims=True)
    clip = jnp.minimum(F32(1.0), F32(max_norm) / (jnp.sqrt(norm_sq) + F32(1e-06)))
    square = clip * clip
    live = clip > 0.0

    def grown(old, mean_square):
        return old + jnp.where(live, square * mean_square, 0.0)

    new_ra = grown(row_ra[...], row_sq[...])
    step = (F32(learn_rate) * clip) * emb_ref[...] / (jnp.sqrt(new_ra) + F32(epsilon))
    rows[...] = row_tab[...] - step
    load.wait()

    def sixteen(i, carry):
        for j in range(16):
            t = i * 16 + j
            tab[pl.ds(idx[t], 1), :] = rows[pl.ds(t, 1), :]
        return carry

    lax.fori_loop(0, 32, sixteen, 0)
    out = [pltpu.make_async_copy(tab, table_out, sems.at[1])]
    out[0].start()
    ra_new[...] = grown(ra_ref[...], flat_sq[...])
    scaled = clip * mean_ref[...]
    grow = acc_ref[...] + scaled * scaled
    dense_acc_new[...] = grow
    dense_new[...] = param_ref[...] - F32(learn_rate) * scaled / (jnp.sqrt(grow) + F32(epsilon))
    for i, (src, dst) in enumerate(
        ((ra_new, row_acc_out), (dense_acc_new, dense_acc_out), (dense_new, dense_out))
    ):
        out.append(pltpu.make_async_copy(src, dst, sems.at[2 + i]))
        out[-1].start()
    for copy in out:
        copy.wait()


def body(dense_grads, dense_param, dense_acc, table, row_acc, touched, emb_grads):
    mean, norm, tab, emb, row_tab, row_sq, row_ra, flat_sq = reduce_mean(
        dense_grads, emb_grads, table, row_acc, touched
    )
    vmem, hbm = pl.BlockSpec(memory_space=pltpu.VMEM), pl.BlockSpec(memory_space=pltpu.HBM)
    shapes = (dense_param.shape, dense_param.shape, table.shape, (32, LANES), table.shape)
    new_dense, new_dense_acc, new_table, new_row_acc, _ = pl.pallas_call(
        update_kernel,
        name="update",
        out_shape=[jax.ShapeDtypeStruct(shape, F32) for shape in shapes],
        in_specs=[vmem] * 11 + [hbm],
        out_specs=[hbm] * 4 + [vmem],
        scratch_shapes=[
            pltpu.SMEM(touched.shape, jnp.int32),
            pltpu.VMEM(emb.shape, F32),
            pltpu.VMEM(dense_param.shape, F32),
            pltpu.VMEM(dense_param.shape, F32),
            pltpu.VMEM((32, LANES), F32),
            pltpu.SemaphoreType.DMA((5,)),
        ],
        input_output_aliases={2: 4},
        compiler_params=pltpu.CompilerParams(vmem_limit_bytes=16 * 1024 * 1024),
    )(
        norm, mean, tab, emb, row_tab, row_sq, row_ra, flat_sq,
        dense_param, dense_acc, row_acc.reshape(32, LANES), touched,
    )
    return (new_dense, new_dense_acc, new_table, new_row_acc.reshape(-1))


def solution(mesh):
    return jax.shard_map(
        body,
        mesh=mesh,
        in_specs=(
            P(("gx", "gy"), None, None),
            P(("gx", "gy"), None),
            P(("gx", "gy"), None),
            P(("gx", "gy"), None),
            P(("gx", "gy")),
            P(("gx", "gy")),
            P(("gx", "gy"), None),
        ),
        out_specs=(
            P(("gx", "gy"), None),
            P(("gx", "gy"), None),
            P(("gx", "gy"), None),
            P(("gx", "gy")),
        ),
        check_vma=False,
    )
```
